256 devices in a mesh: rep: 32 (over x_hi, z, core), tp: 8 (over x_lo, y).
Axes of the slice: x: 4 (x_hi: 2, x_lo: 2; x = x_hi * 2 + x_lo), y: 4, z: 8, core: 2. Of those that a mesh axis runs over, the one named last changes fastest.
Arguments:
- tokens: bfloat16 [32, 1024, 3072], P('rep', 'tp'), may hold values from -100 to 100
- norm_gain: float32 [32, 3072], P('rep'), may hold values from 0.5 to 1.5
- w_query: bfloat16 [32, 3072, 2048], P('rep', None, 'tp'), may hold values from -1 to 1
- key_weight: bfloat16 [32, 3072, 1024], P('rep', None, 'tp'), may hold values from -1 to 1
- value_weight: bfloat16 [32, 3072, 1024], P('rep', None, 'tp'), may hold values from -0.109375 to 0.109375
- attention_gradient: bfloat16 [32, 1024, 2048], P('rep', None, 'tp'), may hold values from -6 to 6
- global_fragment: float32 [512, 3072], P('tp'), may hold values from -6 to 6
- momentum: float32 [512, 3072], P('tp'), may hold values from -3 to 3
- local_fragment: bfloat16 [32, 512, 3072], P('rep', 'tp'), may hold values from -6 to 6
Outputs:
- grad_query_w: bfloat16 [32, 3072, 2048], P('rep', None, 'tp')
- grad_key_w: bfloat16 [32, 3072, 1024], P('rep', None, 'tp')
- grad_value_w: bfloat16 [32, 3072, 1024], P('rep', None, 'tp')
- grad_gain: float32 [32, 3072], P('rep')
- grad_tokens: bfloat16 [32, 1024, 3072], P('rep', 'tp')
- new_global: float32 [512, 3072], P('tp')
- new_momentum: float32 [512, 3072], P('tp')
The draws below stay inside these ranges and needn't reach their ends.
All inputs are finite; a program needn't handle non-finite values.
Results may differ from the reference program's by a relative error of at most 0.019.
The reference program's roundings to bfloat16 on the way count: a program that leaves them out, or rounds other values in their place, can miss the bound.
Values may be sent and summed in bfloat16 or wider, within the bound.
No kernel may reach another device: no remote copies, remote signals or barrier semaphores. Data moves between devices by JAX's collectives and lax.ppermute only.
A program may use at most 128 MiB of HBM per device.

```python
import math
import jax
import jax.numpy as jnp
from jax import lax

MODEL_WIDTH = 3072
QUERY_HEADS = 16
KEY_VALUE_HEADS = 8
HEAD_SIZE = 128
SEQ = 1024
FRAG = 512
N_REP = 32
N_TP = 8


def draw_tokens(key, part):
    col_scale = jnp.exp(jax.random.uniform(jax.random.fold_in(key, 12), (1, 1, MODEL_WIDTH), jnp.float32, math.log(0.5), math.log(2.0)))
    row_scale = jnp.exp(jax.random.uniform(jax.random.fold_in(key, 11), (N_REP, SEQ, 1), jnp.float32, 0.0, math.log(10.0)))
    jitter = jax.random.normal(jax.random.fold_in(key, 13), (N_REP, SEQ, MODEL_WIDTH), jnp.float32)
    result = jitter * col_scale * row_scale
    return jnp.clip(result, -100.0, 100.0).astype(jnp.bfloat16)


def draw_w_query(key, part):
    return (jax.random.normal(jax.random.fold_in(key, 21), (N_REP, MODEL_WIDTH, QUERY_HEADS * HEAD_SIZE), jnp.float32) * MODEL_WIDTH ** (-0.5)).astype(jnp.bfloat16)


def draw_key_weight(key, part):
    return (jax.random.normal(jax.random.fold_in(key, 31), (N_REP, MODEL_WIDTH, KEY_VALUE_HEADS * HEAD_SIZE), jnp.float32) * MODEL_WIDTH ** (-0.5)).astype(jnp.bfloat16)


def levels(own_key, shape, pieces, low, largest):
    level, own = 1.0, jax.random.fold_in(own_key, 6)
    for dim, parts in pieces:
        heights = jnp.exp(jax.random.uniform(jax.random.fold_in(own, dim), (parts,), jnp.float32, low / len(pieces), largest / len(pieces)))
        level = level * jnp.repeat(heights, shape[dim] // parts).reshape([-1 if axis == dim else 1 for axis in range(len(shape))])
    return level


def centred(own_key, shape, spread, reach, cuts=(), kind=jnp.bfloat16):
    array = jax.random.normal(own_key, shape, jnp.float32) * spread
    if len(cuts) > 0:
        array = levels(own_key, shape, cuts, -0.22, 0.18) * array
    return jnp.clip(array, min=-reach, max=reach).astype(kind)


def setup_inputs(seed: int = 0) -> dict:
    seeds = jax.random.split(jax.random.key(seed), 10)
    return {
        "tokens": draw_tokens(jax.random.fold_in(seeds[9], 71), 0),
        "norm_gain": jnp.clip(1.0 + 0.1 * jax.random.normal(seeds[1], (N_REP, MODEL_WIDTH), jnp.float32), 0.5, 1.5),
        "w_query": draw_w_query(jax.random.fold_in(seeds[9], 71), 0),
        "key_weight": draw_key_weight(jax.random.fold_in(seeds[9], 71), 0),
        "value_weight": centred(seeds[4], (N_REP, MODEL_WIDTH, KEY_VALUE_HEADS * HEAD_SIZE), MODEL_WIDTH ** -0.5, 0.109375, ((0, 32), (2, 8))),
        "attention_gradient": centred(seeds[5], (N_REP, SEQ, QUERY_HEADS * HEAD_SIZE), 1.0, 6.0, ((0, 32), (2, 8))),
        "global_fragment": centred(seeds[6], (FRAG, MODEL_WIDTH), 1.0, 6.0, ((0, 8),), jnp.float32),
        "momentum": centred(seeds[7], (FRAG, MODEL_WIDTH), 0.5, 3.0, ((0, 8),), jnp.float32),
        "local_fragment": centred(seeds[8], (N_REP, FRAG, MODEL_WIDTH), 1.0, 6.0, ((0, 32), (1, 8))),
    }


epsilon = 1e-05
rope_base = 500000.0
outer_rate = 0.7
outer_momentum = 0.9

def rope_tables(sequence_length, width):
    middle = width // 2
    frequency = rope_base ** (-2.0 * jnp.arange(middle, dtype=jnp.float32) / width)
    angles = jnp.arange(sequence_length, dtype=jnp.float32)[:, None] * frequency[None, :]
    angles = jnp.concatenate([angles, angles], axis=1)
    return (jnp.cos(angles)[:, None, :], jnp.sin(angles)[:, None, :])

def rotate(vectors, cosine_table, sine_table):
    middle = vectors.shape[-1] // 2
    turned = jnp.concatenate([-vectors[..., middle:], vectors[..., :middle]], axis=-1)
    return vectors * cosine_table + turned * sine_table

def reverse_rotation(gradient, cosine_table, sine_table):
    middle = gradient.shape[-1] // 2
    shifted = gradient * sine_table
    turned = jnp.concatenate([shifted[..., middle:], -shifted[..., :middle]], axis=-1)
    return gradient * cosine_table + turned

def attention_reverse(query_rows, rotated_keys, values_bfloat, grad_out, block_of_rows):
    sequence_length = query_rows.shape[0]
    score_scale = query_rows.shape[-1] ** (-0.5)
    keys_wide = rotated_keys.astype(jnp.float32)
    values_wide = values_bfloat.astype(jnp.float32)

    def one_block(running, block_index):
        acc_key, acc_value = running
        offset = block_index * block_of_rows
        query_block = lax.dynamic_slice_in_dim(query_rows, offset, block_of_rows, 0).astype(jnp.float32)
        grad_block = lax.dynamic_slice_in_dim(grad_out, offset, block_of_rows, 0).astype(jnp.float32)
        scores = jnp.einsum('qgrd,kgd->grqk', query_block, keys_wide) * score_scale
        row_pos = offset + jnp.arange(block_of_rows)
        col_pos = jnp.arange(sequence_length)
        allowed = col_pos[None, :] <= row_pos[:, None]
        scores = jnp.where(allowed, scores, -jnp.inf)
        highest = lax.optimization_barrier(jnp.max(scores, axis=-1, keepdims=True))
        powers = jnp.exp(scores - highest)
        probability = powers / lax.optimization_barrier(jnp.sum(powers, axis=-1, keepdims=True))
        prob_low = lax.optimization_barrier(probability.astype(jnp.bfloat16)).astype(jnp.float32)
        acc_value = acc_value + jnp.einsum('grqk,qgrd->kgd', prob_low, grad_block)
        grad_prob = jnp.einsum('qgrd,kgd->grqk', grad_block, values_wide)
        grad_score = probability * (grad_prob - lax.optimization_barrier(jnp.sum(grad_prob * probability, axis=-1, keepdims=True))) * score_scale
        score_low = lax.optimization_barrier(grad_score.astype(jnp.bfloat16)).astype(jnp.float32)
        grad_query = jnp.einsum('grqk,kgd->qgrd', score_low, keys_wide)
        acc_key = acc_key + jnp.einsum('grqk,qgrd->kgd', score_low, query_block)
        return ((acc_key, acc_value), grad_query)
    initial = jnp.zeros(rotated_keys.shape, jnp.float32)
    (acc_key, acc_value), grad_blocks = lax.scan(one_block, (initial, initial), jnp.arange(sequence_length // block_of_rows))
    grad_query = grad_blocks.reshape(query_rows.shape)
    return (grad_query, acc_key, acc_value)

def replica_grads(items):
    tokens, norm_gains, w_query, key_weight, value_weight, attention_gradient = items
    sequence_length = tokens.shape[0]
    widened_rows = tokens.astype(jnp.float32)
    inverse_norm = lax.rsqrt(lax.optimization_barrier(jnp.mean(widened_rows * widened_rows, axis=-1, keepdims=True)) + epsilon)
    normalized_input = widened_rows * inverse_norm
    normalized = (normalized_input * norm_gains[None, :]).astype(jnp.bfloat16)
    cosine_table, sine_table = rope_tables(sequence_length, HEAD_SIZE)
    query_rows = jnp.dot(normalized, w_query, preferred_element_type=jnp.float32).reshape(sequence_length, QUERY_HEADS, HEAD_SIZE)
    query_rows = rotate(query_rows, cosine_table, sine_table).astype(jnp.bfloat16)
    rotated_keys = jnp.dot(normalized, key_weight, preferred_element_type=jnp.float32).reshape(sequence_length, KEY_VALUE_HEADS, HEAD_SIZE)
    rotated_keys = rotate(rotated_keys, cosine_table, sine_table).astype(jnp.bfloat16)
    values_bfloat = jnp.dot(normalized, value_weight, preferred_element_type=jnp.float32).astype(jnp.bfloat16).reshape(sequence_length, KEY_VALUE_HEADS, HEAD_SIZE)
    replica_group = QUERY_HEADS // KEY_VALUE_HEADS
    block_of_rows = min(512, sequence_length)
    query_input_gradient, key_input_gradient, value_input_gradient = attention_reverse(query_rows.reshape(sequence_length, KEY_VALUE_HEADS, replica_group, HEAD_SIZE), rotated_keys, values_bfloat, attention_gradient.reshape(sequence_length, KEY_VALUE_HEADS, replica_group, HEAD_SIZE), block_of_rows)
    dquery = reverse_rotation(query_input_gradient.reshape(sequence_length, QUERY_HEADS, HEAD_SIZE), cosine_table, sine_table).astype(jnp.bfloat16).reshape(sequence_length, QUERY_HEADS * HEAD_SIZE)
    key_gradient = reverse_rotation(key_input_gradient, cosine_table, sine_table).astype(jnp.bfloat16).reshape(sequence_length, KEY_VALUE_HEADS * HEAD_SIZE)
    value_gradient = value_input_gradient.astype(jnp.bfloat16).reshape(sequence_length, KEY_VALUE_HEADS * HEAD_SIZE)
    contract = (((0,), (0,)), ((), ()))
    grad_wq = lax.dot_general(normalized, dquery, contract, preferred_element_type=jnp.float32).astype(jnp.bfloat16)
    grad_wk = lax.dot_general(normalized, key_gradient, contract, preferred_element_type=jnp.float32).astype(jnp.bfloat16)
    grad_wv = lax.dot_general(normalized, value_gradient, contract, preferred_element_type=jnp.float32).astype(jnp.bfloat16)
    query_cols = QUERY_HEADS * HEAD_SIZE // N_TP
    key_value_columns = KEY_VALUE_HEADS * HEAD_SIZE // N_TP
    back = (((1,), (1,)), ((), ()))
    summed_rows = jnp.zeros((sequence_length, MODEL_WIDTH), jnp.float32)
    for shard_index in range(N_TP):
        qa, qb_end = (shard_index * query_cols, (shard_index + 1) * query_cols)
        ka, kb_end = (shard_index * key_value_columns, (shard_index + 1) * key_value_columns)
        partial_value = lax.dot_general(dquery[:, qa:qb_end], w_query[:, qa:qb_end], back, preferred_element_type=jnp.float32)
        partial_value = partial_value + lax.dot_general(key_gradient[:, ka:kb_end], key_weight[:, ka:kb_end], back, preferred_element_type=jnp.float32)
        partial_value = partial_value + lax.dot_general(value_gradient[:, ka:kb_end], value_weight[:, ka:kb_end], back, preferred_element_type=jnp.float32)
        summed_rows = summed_rows + lax.optimization_barrier(partial_value.astype(jnp.bfloat16)).astype(jnp.float32)
    gains_gradient = lax.optimization_barrier(jnp.sum(summed_rows * normalized_input, axis=0))
    scaled_rows = summed_rows * norm_gains[None, :]
    gradient_rows = inverse_norm * (scaled_rows - normalized_input * lax.optimization_barrier(jnp.mean(scaled_rows * normalized_input, axis=-1, keepdims=True)))
    return (grad_wq, grad_wk, grad_wv, gains_gradient, gradient_rows.astype(jnp.bfloat16))

def reference(tokens, norm_gain, w_query, key_weight, value_weight, attention_gradient, global_fragment, momentum, local_fragment):
    grad_wq, grad_wk, grad_wv, gains_gradient, gradient_rows = lax.map(replica_grads, (tokens, norm_gain, w_query, key_weight, value_weight, attention_gradient))
    delta = global_fragment[None, :, :] - local_fragment.astype(jnp.float32)
    mean_delta = lax.optimization_barrier(jnp.sum(delta, axis=0)) / N_REP
    new_momentum = outer_momentum * momentum + mean_delta
    new_global = global_fragment - outer_rate * (mean_delta + outer_momentum * new_momentum)
    return (grad_wq, grad_wk, grad_wv, gains_gradient, gradient_rows, new_global, new_momentum)
```

```python
import functools

import jax
import jax.numpy as jnp
from jax import lax
from jax.experimental import pallas as pl
from jax.experimental.pallas import tpu as pltpu
from jax.sharding import PartitionSpec as P

HEAD_SIZE = 128
A = 1792
MODEL = 3072
B = MODEL - A
H = A // 2
HB = B // 2
ROWS = 128
SEQ = 1024
TILE = 256

epsilon = 1e-05
rope_base = 500000.0
outer_rate = 0.7
outer_momentum = 0.9


f32 = jnp.float32
bf16 = jnp.bfloat16
NT = (((1,), (1,)), ((), ()))
TN = (((0,), (0,)), ((), ()))
NN = (((1,), (0,)), ((), ()))

BLOCKS = ((0, 0), (1, 0), (0, -1), (0, 1), (1, -1), (1, 1), (0, 2), (1, 2))
WHERE = {block: at for at, block in enumerate(BLOCKS)}


def index(x, y):
    return x * 4 + y % 4


X_PAIRS = [(index(x, y), index(1 - x, y)) for x in range(2) for y in range(4)]
UP_PAIRS = [(index(x, y), index(x, y + 1)) for x in range(2) for y in range(4)]
DOWN_PAIRS = [(index(x, y), index(x, y - 1)) for x in range(2) for y in range(4)]


def across(value):
    return lax.ppermute(value, "tp", X_PAIRS)


def up(value):
    return lax.ppermute(value, "tp", UP_PAIRS)


def down(value):
    return lax.ppermute(value, "tp", DOWN_PAIRS)


def dot(a, b, dims):
    return lax.dot_general(a, b, dims, preferred_element_type=f32)


VM = pl.BlockSpec(memory_space=pltpu.VMEM)
SM = pl.BlockSpec(memory_space=pltpu.SMEM)


def call(kernel, outs, ins, flops, scratch=(), smem=0):
    nbytes = sum(v.size * v.dtype.itemsize for v in ins) + sum(
        o.size * o.dtype.itemsize for o in outs
    )
    return pl.pallas_call(
        kernel,
        out_shape=tuple(outs),
        in_specs=[SM] * smem + [VM] * (len(ins) - smem),
        out_specs=tuple([VM] * len(outs)),
        scratch_shapes=list(scratch),
        cost_estimate=pl.CostEstimate(flops=flops, bytes_accessed=nbytes, transcendentals=0),
        compiler_params=pltpu.CompilerParams(vmem_limit_bytes=48 * 1024 * 1024),
    )(*ins)


def shape(*dims, dtype=bf16):
    return jax.ShapeDtypeStruct(dims, dtype)


def norm_kernel(tokens, gain, part_a, part_b):
    wide = tokens[...].astype(f32)
    inverse = lax.rsqrt(jnp.mean(wide * wide, axis=-1, keepdims=True) + epsilon)
    part_a[...] = (wide[:, :A] * inverse * gain[:, :A]).astype(bf16)
    part_b[...] = (wide[:, A:] * inverse * gain[:, A:]).astype(bf16)


def project_kernel(n, split, *refs):
    parts_a = refs[:n]
    count_b = 2 * n if split else n
    parts_b = refs[n : n + count_b]
    wq, wk, wv, out = refs[n + count_b :]
    rows_a = jnp.concatenate([r[...] for r in parts_a], axis=0)
    if split:
        blocks = [
            jnp.concatenate([parts_b[2 * i][...], parts_b[2 * i + 1][...]], axis=1)
            for i in range(n)
        ]
    else:
        blocks = [r[...] for r in parts_b]
    rows_b = jnp.concatenate(blocks, axis=0)
    out[:, :256] = dot(rows_a, wq[:A, :], NN) + dot(rows_b, wq[A:, :], NN)
    both = jnp.concatenate([wk[...], wv[...]], axis=1)
    out[:, 256:] = dot(rows_a, both[:A, :], NN) + dot(rows_b, both[A:, :], NN)


def sign_row():
    lane = lax.broadcasted_iota(jnp.int32, (1, HEAD_SIZE), 1)
    return jnp.where(lane < HEAD_SIZE // 2, -1.0, 1.0).astype(f32)


def attention_kernel(at, first, second, third, cosine, sine, grad_out, out, qs, ks, vs, dk, dv):
    sign = sign_row()
    scale = HEAD_SIZE ** (-0.5)

    def rotate(v, c, s):
        return v * c + pltpu.roll(v, HEAD_SIZE // 2, 1) * (sign * s)

    def rotate_back(g, c, s):
        return g * c - pltpu.roll(g * s, HEAD_SIZE // 2, 1) * sign

    for j in range(8):
        if j < 4:
            source, base = first, j * ROWS
        elif j < 6:
            source, base = second, (j - 4) * ROWS
        else:
            source, base = third, (j - 6) * ROWS
        here = pl.ds(pl.multiple_of(at[j] * ROWS, ROWS), ROWS)
        c, s = cosine[here, :], sine[here, :]
        block = source[base : base + ROWS, :]
        qs[here, :128] = rotate(block[:, :128], c, s).astype(bf16)
        qs[here, 128:] = rotate(block[:, 128:256], c, s).astype(bf16)
        ks[here, :] = rotate(block[:, 256:384], c, s).astype(bf16)
        vs[here, :] = block[:, 384:].astype(bf16)

    dk[...] = jnp.zeros_like(dk)
    dv[...] = jnp.zeros_like(dv)
    key_at = lax.broadcasted_iota(jnp.int32, (TILE, TILE), 0)
    query_at = lax.broadcasted_iota(jnp.int32, (TILE, TILE), 1)
    allowed = key_at <= query_at
    for i in range(SEQ // TILE):
        lo, hi = i * TILE, (i + 1) * TILE
        keys, values = ks[:hi, :], vs[:hi, :]
        for h in range(2):
            cols = slice(h * 128, (h + 1) * 128)
            q, g = qs[lo:hi, cols], grad_out[lo:hi, cols]
            scores = dot(keys, q, NT) * scale
            last = jnp.where(allowed, scores[lo:, :], -jnp.inf)
            scores = jnp.concatenate([scores[:lo, :], last], axis=0) if i else last
            powers = jnp.exp(scores - jnp.max(scores, axis=0, keepdims=True))
            probability = powers * (1.0 / jnp.sum(powers, axis=0, keepdims=True))
            dv[:hi, :] += dot(probability.astype(bf16), g, NN)
            grad_prob = dot(values, g, NT)
            row = jnp.sum(grad_prob * probability, axis=0, keepdims=True)
            grad_score = (probability * (grad_prob - row) * scale).astype(bf16)
            dk[:hi, :] += dot(grad_score, q, NN)
            dq = dot(grad_score, keys, TN)
            out[lo:hi, cols] = rotate_back(dq, cosine[lo:hi, :], sine[lo:hi, :]).astype(bf16)
    out[:, 256:384] = rotate_back(dk[...], cosine[...], sine[...]).astype(bf16)
    out[:, 384:] = dv[...].astype(bf16)


def rows_of(at, ref, block):
    return ref[pl.ds(pl.multiple_of(at[WHERE[block]] * ROWS, ROWS), ROWS), :]


def back_tile(rows, wq, wk, wv, cols):
    both = jnp.concatenate([wk[cols, :], wv[cols, :]], axis=1)
    return (dot(rows[:, :256], wq[cols, :], NT) + dot(rows[:, 256:], both, NT)).astype(bf16)


def first_back_kernel(at, grads, wq, wk, wv, far_low, far_high, x2, x1, xm, x0):
    far = jnp.concatenate([rows_of(at, grads, (0, 2)), rows_of(at, grads, (1, 2))], axis=0)
    for i in range(0, A, 128):
        tile = back_tile(far, wq, wk, wv, slice(i, i + 128))
        if i < H:
            far_low[:, i : i + 128] = tile
        else:
            far_high[:, i - H : i - H + 128] = tile
    other = jnp.concatenate([rows_of(at, grads, (1, d)) for d in (2, 1, -1, 0)], axis=0)
    for i in range(0, B, 256):
        tile = back_tile(other, wq, wk, wv, slice(A + i, A + i + 256))
        for n, ref in enumerate((x2, x1, xm, x0)):
            ref[:, i : i + 256] = tile[n * ROWS : (n + 1) * ROWS, :]


def second_back_kernel(
    at, grads, wq, wk, wv, up_low, up_high, down_low, down_high, own_a, q2, q1, qm, q0
):
    near = jnp.concatenate(
        [rows_of(at, grads, (x, d)) for d in (1, -1, 0) for x in (0, 1)], axis=0
    )
    for i in range(0, A, 128):
        tile = back_tile(near, wq, wk, wv, slice(i, i + 128))
        low = i < H
        col = i if low else i - H
        (up_low if low else up_high)[:, col : col + 128] = tile[:256, :]
        (down_low if low else down_high)[:, col : col + 128] = tile[256:512, :]
        own_a[:, i : i + 128] = tile[512:, :]
    mine = jnp.concatenate([rows_of(at, grads, (0, d)) for d in (2, 1, -1, 0)], axis=0)
    for i in range(0, B, 256):
        tile = back_tile(mine, wq, wk, wv, slice(A + i, A + i + 256))
        for n, ref in enumerate((q2, q1, qm, q0)):
            ref[:, i : i + 256] = tile[n * ROWS : (n + 1) * ROWS, :]


def weight_kernel(at, *refs):
    parts_a, parts_b, halves = refs[:8], refs[8:14], refs[14:18]
    grads, wq, wk, wv, gain, dwq, dwk, dwv, gain_part, ordered, last = refs[18:]
    for j in range(8):
        ordered[j * ROWS : (j + 1) * ROWS, :] = grads[
            pl.ds(pl.multiple_of(at[j] * ROWS, ROWS), ROWS), :
        ]
    for j in range(2):
        last[j * ROWS : (j + 1) * ROWS, :HB] = halves[2 * j][...]
        last[j * ROWS : (j + 1) * ROWS, HB:] = halves[2 * j + 1][...]

    def tile(rows, to):
        product = dot(rows, ordered[...], TN)
        where = pl.ds(to, 256)
        dwq[where, :] = product[:, :256].astype(bf16)
        dwk[where, :] = product[:, 256:384].astype(bf16)
        dwv[where, :] = product[:, 384:].astype(bf16)
        total = (
            product[:, :128] * wq[where, :128].astype(f32)
            + product[:, 128:256] * wq[where, 128:].astype(f32)
            + product[:, 256:384] * wk[where, :].astype(f32)
            + product[:, 384:] * wv[where, :].astype(f32)
        )
        gain_part[:, where] = jnp.sum(total.T, axis=0, keepdims=True) / gain[:, where]

    @pl.loop(0, A // 256)
    def _(i):
        col = pl.multiple_of(i * 256, 256)
        tile(jnp.concatenate([r[:, pl.ds(col, 256)] for r in parts_a], axis=0), col)

    @pl.loop(0, B // 256)
    def _(i):
        col = pl.multiple_of(i * 256, 256)
        rows = [r[:, pl.ds(col, 256)] for r in parts_b] + [last[:, pl.ds(col, 256)]]
        tile(jnp.concatenate(rows, axis=0), pl.multiple_of(A + col, 256))


def token_kernel(tokens, gain, own_a, from_x, own_b, from_below, from_above, out):
    wide = tokens[...].astype(f32)
    inverse = lax.rsqrt(jnp.mean(wide * wide, axis=-1, keepdims=True) + epsilon)
    hat = wide * inverse
    sum_a = own_a[...] + from_x[...].astype(f32)
    sum_b = own_b[...] + from_below[...].astype(f32) + from_above[...].astype(f32)
    scaled_a = sum_a * gain[:, :A]
    scaled_b = sum_b * gain[:, A:]
    mean = (
        jnp.sum(scaled_a * hat[:, :A], axis=-1, keepdims=True)
        + jnp.sum(scaled_b * hat[:, A:], axis=-1, keepdims=True)
    ) / MODEL
    out[:, :A] = (inverse * (scaled_a - hat[:, :A] * mean)).astype(bf16)
    out[:, A:] = (inverse * (scaled_b - hat[:, A:] * mean)).astype(bf16)


def rope_tables(sequence_length, width):
    middle = width // 2
    frequency = rope_base ** (-2.0 * jnp.arange(middle, dtype=f32) / width)
    angles = jnp.arange(sequence_length, dtype=f32)[:, None] * frequency[None, :]
    cosine, sine = jnp.cos(angles), jnp.sin(angles)
    return (
        jnp.concatenate([cosine, cosine], axis=1),
        jnp.concatenate([sine, sine], axis=1),
    )


def sent_to_all(value, axis):
    copies = jnp.broadcast_to(value, (lax.axis_size(axis), *value.shape))
    return lax.all_to_all(copies, axis, split_axis=0, concat_axis=0, tiled=True)


def add(a, b):
    return (a.astype(f32) + b.astype(f32)).astype(bf16)


def body(
    tokens,
    norm_gain,
    w_query,
    key_weight,
    value_weight,
    attention_gradient,
    global_fragment,
    momentum,
    local_fragment,
):
    rows = tokens[0]
    wq, wk, wv = w_query[0], key_weight[0], value_weight[0]
    me = lax.axis_index("tp")
    step_x = jnp.array([b[0] for b in BLOCKS], jnp.int32)
    step_y = jnp.array([b[1] for b in BLOCKS], jnp.int32)
    at = ((me // 4 + step_x) % 2) * 4 + (me % 4 + step_y + 4) % 4

    a00, b00 = call(norm_kernel, [shape(ROWS, A), shape(ROWS, B)], [rows, norm_gain], 10**6)
    a10 = across(a00)
    bm = up(b00)
    bp = down(b00)
    am = up(a00)
    ap = down(a00)
    b10 = across(b00)
    b2l = up(bm[:, :HB])
    b2h = down(bp[:, HB:])
    b1m = across(bm)
    b1p = across(bp)
    a1m = up(a10)
    a1p = down(a10)
    b12l = across(b2l)
    b12h = across(b2h)
    a02 = up(am)
    a12 = down(a1p)

    parts_a = [a00, a10, am, ap, a1m, a1p, a02, a12]
    parts_b = [b00, b10, bm, bp, b1m, b1p]
    halves = [b2l, b2h, b12l, b12h]
    weights = [wq, wk, wv]
    (first,) = call(
        functools.partial(project_kernel, 4, False),
        [shape(512, 512, dtype=f32)],
        parts_a[:4] + parts_b[:4] + weights,
        2 * 512 * 512 * MODEL,
    )
    (second,) = call(
        functools.partial(project_kernel, 2, False),
        [shape(256, 512, dtype=f32)],
        parts_a[4:6] + parts_b[4:6] + weights,
        2 * 256 * 512 * MODEL,
    )
    (third,) = call(
        functools.partial(project_kernel, 2, True),
        [shape(256, 512, dtype=f32)],
        parts_a[6:] + halves + weights,
        2 * 256 * 512 * MODEL,
    )
    cosine, sine = rope_tables(SEQ, HEAD_SIZE)
    (grads,) = call(
        attention_kernel,
        [shape(SEQ, 512)],
        [at, first, second, third, cosine, sine, attention_gradient[0]],
        10 * SEQ * SEQ * 256,
        scratch=[
            pltpu.VMEM((SEQ, 256), bf16),
            pltpu.VMEM((SEQ, 128), bf16),
            pltpu.VMEM((SEQ, 128), bf16),
            pltpu.VMEM((SEQ, 128), f32),
            pltpu.VMEM((SEQ, 128), f32),
        ],
        smem=1,
    )
    far_low, far_high, x2, x1, xm, x0 = call(
        first_back_kernel,
        [shape(256, H), shape(256, H)] + [shape(ROWS, B)] * 4,
        [at, grads] + weights,
        2 * 512 * (256 * A + 512 * B),
        smem=1,
    )
    near_low = up(far_low)
    near_high = down(far_high)
    r2 = across(x2)
    r1 = across(x1)
    rm = across(xm)
    r0 = across(x0)
    up_low, up_high, down_low, down_high, own_a, q2, q1, qm, q0 = call(
        second_back_kernel,
        [shape(256, H)] * 4 + [shape(256, A)] + [shape(ROWS, B)] * 4,
        [at, grads] + weights,
        2 * 512 * (768 * A + 512 * B),
        smem=1,
    )
    below_high = up(up_high)
    above_low = down(down_low)
    far_b = add(q2, r2)
    near_b_low = up(far_b[:, :HB])
    near_b_high = down(far_b[:, HB:])
    below_low = up(add(up_low, near_low))
    above_high = down(add(down_high, near_high))
    summed_low = own_a[:, :H].astype(f32) + below_low.astype(f32) + above_low.astype(f32)
    summed_high = own_a[:, H:].astype(f32) + below_high.astype(f32) + above_high.astype(f32)
    summed = jnp.concatenate([summed_low, summed_high], axis=1)
    from_x = across(summed[ROWS:].astype(bf16))
    b_up = q1.astype(f32) + r1.astype(f32)
    b_up = jnp.concatenate([b_up[:, :HB] + near_b_low.astype(f32), b_up[:, HB:]], axis=1)
    b_down = qm.astype(f32) + rm.astype(f32)
    b_down = jnp.concatenate([b_down[:, :HB], b_down[:, HB:] + near_b_high.astype(f32)], axis=1)
    from_below = up(b_up.astype(bf16))
    from_above = down(b_down.astype(bf16))
    own_b = q0.astype(f32) + r0.astype(f32)

    grad_wq, grad_wk, grad_wv, gain_part = call(
        weight_kernel,
        [shape(MODEL, 256), shape(MODEL, 128), shape(MODEL, 128), shape(1, MODEL, dtype=f32)],
        [at] + parts_a + parts_b + halves + [grads] + weights + [norm_gain],
        2 * SEQ * 512 * MODEL,
        scratch=[pltpu.VMEM((SEQ, 512), bf16), pltpu.VMEM((256, B), bf16)],
        smem=1,
    )
    grad_gain = jnp.sum(sent_to_all(gain_part, "tp"), axis=0)
    (grad_rows,) = call(
        token_kernel,
        [shape(ROWS, MODEL)],
        [rows, norm_gain, summed[:ROWS], from_x, own_b, from_below, from_above],
        10**6,
    )

    replicas = lax.axis_size("rep")
    count = global_fragment.shape[0] // replicas
    parts = local_fragment[0].reshape(replicas, count, MODEL)
    arrived = lax.all_to_all(parts, "rep", split_axis=0, concat_axis=0, tiled=True)
    offset = lax.axis_index("rep") * count
    global_rows = lax.dynamic_slice_in_dim(global_fragment, offset, count, 0)
    mean_rows = jnp.sum(global_rows[None] - arrived.astype(f32), axis=0) / replicas
    mean = sent_to_all(mean_rows, "rep").reshape(global_fragment.shape)
    new_momentum = outer_momentum * momentum + mean
    new_global = global_fragment - outer_rate * (mean + outer_momentum * new_momentum)
    return (
        grad_wq[None],
        grad_wk[None],
        grad_wv[None],
        grad_gain,
        grad_rows[None],
        new_global,
        new_momentum,
    )


def solution(mesh):
    placed = (
        P("rep", "tp", None),
        P("rep", None),
        P("rep", None, "tp"),
        P("rep", None, "tp"),
        P("rep", None, "tp"),
        P("rep", None, "tp"),
        P("tp", None),
        P("tp", None),
        P("rep", "tp", None),
    )

    return jax.shard_map(
        body,
        mesh=mesh,
        in_specs=placed,
        out_specs=(
            P("rep", None, "tp"),
            P("rep", None, "tp"),
            P("rep", None, "tp"),
            P("rep", None),
            P("rep", "tp", None),
            P("tp", None),
            P("tp", None),
        ),
        check_vma=False,
    )
```

```python
import functools

import jax
import jax.numpy as jnp
from jax import lax
from jax.experimental import pallas as pl
from jax.experimental.pallas import tpu as pltpu
from jax.sharding import PartitionSpec as P


HEAD_SIZE = 128
A = 1792
MODEL = 3072
B = MODEL - A
HB = B // 2
SA = 1664
SB = MODEL - SA
SH = 896
SHB = 640
ROWS = 128
SEQ = 1024
TILE = 256
STEP_A = 896
STEP_B = 640

epsilon = 1e-05
rope_base = 500000.0
outer_rate = 0.7
outer_momentum = 0.9


f32 = jnp.float32
bf16 = jnp.bfloat16
NT = (((1,), (1,)), ((), ()))
TN = (((0,), (0,)), ((), ()))
NN = (((1,), (0,)), ((), ()))

BLOCKS = ((0, 0), (1, 0), (0, -1), (0, 1), (1, -1), (1, 1), (0, 2), (1, 2))
WHERE = {block: at for at, block in enumerate(BLOCKS)}


def index(x, y):
    return x * 4 + y % 4


X_PAIRS = [(index(x, y), index(1 - x, y)) for x in range(2) for y in range(4)]
UP_PAIRS = [(index(x, y), index(x, y + 1)) for x in range(2) for y in range(4)]
DOWN_PAIRS = [(index(x, y), index(x, y - 1)) for x in range(2) for y in range(4)]


def across(value):
    return lax.ppermute(value, "tp", X_PAIRS)


def up(value):
    return lax.ppermute(value, "tp", UP_PAIRS)


def down(value):
    return lax.ppermute(value, "tp", DOWN_PAIRS)


def dot(a, b, dims):
    return lax.dot_general(a, b, dims, preferred_element_type=f32)


VMEM_LIMIT = {"attention": 16, "weights": 16, "project_first": 16}
VM = pl.BlockSpec(memory_space=pltpu.VMEM)
SM = pl.BlockSpec(memory_space=pltpu.SMEM)


def call(kernel, name, outs, ins, flops, scratch=(), smem=0):
    nbytes = sum(v.size * v.dtype.itemsize for v in ins) + sum(
        o.size * o.dtype.itemsize for o in outs
    )
    return pl.pallas_call(
        kernel,
        out_shape=tuple(outs),
        in_specs=[SM] * smem + [VM] * (len(ins) - smem),
        out_specs=tuple([VM] * len(outs)),
        scratch_shapes=list(scratch),
        cost_estimate=pl.CostEstimate(flops=flops, bytes_accessed=nbytes, transcendentals=0),
        compiler_params=pltpu.CompilerParams(vmem_limit_bytes=VMEM_LIMIT.get(name, 8) * 1024 * 1024),
    )(*ins)


def shape(*dims, dtype=bf16):
    return jax.ShapeDtypeStruct(dims, dtype)


def norm_kernel(tokens, gain, part_a, part_b):
    wide = tokens[...].astype(f32)
    inverse = lax.rsqrt(jnp.mean(wide * wide, axis=-1, keepdims=True) + epsilon)
    part_a[...] = (wide[:, :A] * inverse * gain[:, :A]).astype(bf16)
    part_b[...] = (wide[:, A:] * inverse * gain[:, A:]).astype(bf16)


def project_kernel(n, split, *refs):
    parts_a = refs[:n]
    count_b = 2 * n if split else n
    parts_b = refs[n : n + count_b]
    wq, wk, wv, out = refs[n + count_b :]
    rows_a = jnp.concatenate([r[...] for r in parts_a], axis=0)
    if split:
        blocks = [
            jnp.concatenate([parts_b[2 * i][...], parts_b[2 * i + 1][...]], axis=1)
            for i in range(n)
        ]
    else:
        blocks = [r[...] for r in parts_b]
    rows_b = jnp.concatenate(blocks, axis=0)
    out[:, :256] = dot(rows_a, wq[:A, :], NN) + dot(rows_b, wq[A:, :], NN)
    both = jnp.concatenate([wk[...], wv[...]], axis=1)
    out[:, 256:] = dot(rows_a, both[:A, :], NN) + dot(rows_b, both[A:, :], NN)


def sign_row():
    lane = lax.broadcasted_iota(jnp.int32, (1, HEAD_SIZE), 1)
    return jnp.where(lane < HEAD_SIZE // 2, -1.0, 1.0).astype(f32)


def attention_kernel(at, first, second, third, cosine, sine, grad_out, out, qs, ks, vs, dk, dv):
    sign = sign_row()
    scale = HEAD_SIZE ** (-0.5)

    def rotate(v, c, s):
        return v * c + pltpu.roll(v, HEAD_SIZE // 2, 1) * (sign * s)

    def rotate_back(g, c, s):
        return g * c - pltpu.roll(g * s, HEAD_SIZE // 2, 1) * sign

    for j in range(8):
        if j < 4:
            source, base = first, j * ROWS
        elif j < 6:
            source, base = second, (j - 4) * ROWS
        else:
            source, base = third, (j - 6) * ROWS
        here = pl.ds(pl.multiple_of(at[j] * ROWS, ROWS), ROWS)
        c, s = cosine[here, :], sine[here, :]
        block = source[base : base + ROWS, :]
        qs[here, :128] = rotate(block[:, :128], c, s).astype(bf16)
        qs[here, 128:] = rotate(block[:, 128:256], c, s).astype(bf16)
        ks[here, :] = rotate(block[:, 256:384], c, s).astype(bf16)
        vs[here, :] = block[:, 384:].astype(bf16)

    dk[...] = jnp.zeros_like(dk)
    dv[...] = jnp.zeros_like(dv)
    key_at = lax.broadcasted_iota(jnp.int32, (TILE, TILE), 0)
    query_at = lax.broadcasted_iota(jnp.int32, (TILE, TILE), 1)
    allowed = key_at <= query_at
    for i in range(SEQ // TILE):
        lo, hi = i * TILE, (i + 1) * TILE
        keys, values = ks[:hi, :], vs[:hi, :]
        for h in range(2):
            cols = slice(h * 128, (h + 1) * 128)
            q, g = qs[lo:hi, cols], grad_out[lo:hi, cols]
            scores = dot(keys, q, NT) * scale
            last = jnp.where(allowed, scores[lo:, :], -jnp.inf)
            scores = jnp.concatenate([scores[:lo, :], last], axis=0) if i else last
            powers = jnp.exp(scores - jnp.max(scores, axis=0, keepdims=True))
            probability = powers * (1.0 / jnp.sum(powers, axis=0, keepdims=True))
            dv[:hi, :] += dot(probability.astype(bf16), g, NN)
            grad_prob = dot(values, g, NT)
            row = jnp.sum(grad_prob * probability, axis=0, keepdims=True)
            grad_score = (probability * (grad_prob - row) * scale).astype(bf16)
            dk[:hi, :] += dot(grad_score, q, NN)
            dq = dot(grad_score, keys, TN)
            out[lo:hi, cols] = rotate_back(dq, cosine[lo:hi, :], sine[lo:hi, :]).astype(bf16)
    out[:, 256:384] = rotate_back(dk[...], cosine[...], sine[...]).astype(bf16)
    out[:, 384:] = dv[...].astype(bf16)


def rows_of(at, ref, block):
    return ref[pl.ds(pl.multiple_of(at[WHERE[block]] * ROWS, ROWS), ROWS), :]


def back_tile(rows, wq, wk, wv, cols):
    both = jnp.concatenate([wk[cols, :], wv[cols, :]], axis=1)
    return (dot(rows[:, :256], wq[cols, :], NT) + dot(rows[:, 256:], both, NT)).astype(bf16)


def pieces(start, stop):
    return [(i, min(i + 256, stop)) for i in range(start, stop, 256)]


def far_back_kernel(at, grads, wq, wk, wv, far_low, far_high):
    far = jnp.concatenate([rows_of(at, grads, (0, 2)), rows_of(at, grads, (1, 2))], axis=0)
    for i, j in pieces(0, SH):
        far_low[:, i:j] = back_tile(far, wq, wk, wv, slice(i, j))
    for i, j in pieces(SH, SA):
        far_high[:, i - SH : j - SH] = back_tile(far, wq, wk, wv, slice(i, j))


def other_back_kernel(at, grads, wq, wk, wv, x2, x1m, x0):
    other = jnp.concatenate([rows_of(at, grads, (1, d)) for d in (2, 1, -1, 0)], axis=0)
    for i, j in pieces(0, SB):
        tile = back_tile(other, wq, wk, wv, slice(SA + i, SA + j))
        x2[:, i:j] = tile[:ROWS, :]
        x1m[:, i:j] = tile[ROWS : 3 * ROWS, :]
        x0[:, i:j] = tile[3 * ROWS :, :]


def near_back_kernel(
    at, grads, wq, wk, wv, up_low, up_high, down_low, down_high, own_a, q2, q1, qm, q0
):
    near = jnp.concatenate(
        [rows_of(at, grads, (x, d)) for d in (1, -1, 0) for x in (0, 1)], axis=0
    )
    for base, end, above, below in ((0, SH, up_low, down_low), (SH, SA, up_high, down_high)):
        for i, j in pieces(base, end):
            tile = back_tile(near, wq, wk, wv, slice(i, j))
            above[:, i - base : j - base] = tile[:256, :]
            below[:, i - base : j - base] = tile[256:512, :]
            own_a[:, i:j] = tile[512:, :]
    mine = jnp.concatenate([rows_of(at, grads, (0, d)) for d in (2, 1, -1, 0)], axis=0)
    for i, j in pieces(0, SB):
        tile = back_tile(mine, wq, wk, wv, slice(SA + i, SA + j))
        for n, ref in enumerate((q2, q1, qm, q0)):
            ref[:, i:j] = tile[n * ROWS : (n + 1) * ROWS, :]


def weight_kernel(at, *refs):
    parts_a, parts_b, halves = refs[:8], refs[8:14], refs[14:18]
    grads, wq, wk, wv, gain, dwq, dwk, dwv, gain_part, ordered, last = refs[18:]
    for j in range(8):
        ordered[j * ROWS : (j + 1) * ROWS, :] = grads[
            pl.ds(pl.multiple_of(at[j] * ROWS, ROWS), ROWS), :
        ]
    for j in range(2):
        last[j * ROWS : (j + 1) * ROWS, :HB] = halves[2 * j][...]
        last[j * ROWS : (j + 1) * ROWS, HB:] = halves[2 * j + 1][...]

    def tile(rows, to, size):
        product = dot(rows, ordered[...], TN)
        where = pl.ds(to, size)
        dwq[where, :] = product[:, :256].astype(bf16)
        dwk[where, :] = product[:, 256:384].astype(bf16)
        dwv[where, :] = product[:, 384:].astype(bf16)
        total = (
            product[:, :128] * wq[where, :128].astype(f32)
            + product[:, 128:256] * wq[where, 128:].astype(f32)
            + product[:, 256:384] * wk[where, :].astype(f32)
            + product[:, 384:] * wv[where, :].astype(f32)
        )
        gain_part[:, where] = jnp.sum(total.T, axis=0, keepdims=True) / gain[:, where]

    @pl.loop(0, A // STEP_A)
    def _(i):
        col = pl.multiple_of(i * STEP_A, 128)
        rows = [r[:, pl.ds(col, STEP_A)] for r in parts_a]
        tile(jnp.concatenate(rows, axis=0), col, STEP_A)

    @pl.loop(0, B // STEP_B)
    def _(i):
        col = pl.multiple_of(i * STEP_B, 128)
        rows = [r[:, pl.ds(col, STEP_B)] for r in parts_b] + [last[:, pl.ds(col, STEP_B)]]
        tile(jnp.concatenate(rows, axis=0), pl.multiple_of(A + col, 128), STEP_B)


def far_sum_kernel(mine, arrived, low, high):
    total = (mine[...].astype(f32) + arrived[...].astype(f32)).astype(bf16)
    low[...] = total[:, :SHB]
    high[...] = total[:, SHB:]


def near_sum_kernel(up_low, near_low, down_high, near_high, to_up, to_down):
    to_up[...] = (up_low[...].astype(f32) + near_low[...].astype(f32)).astype(bf16)
    to_down[...] = (down_high[...].astype(f32) + near_high[...].astype(f32)).astype(bf16)


def b_sum_kernel(q1, qm, r, near_low, near_high, to_up, to_down):
    low, high = slice(0, SHB), slice(SHB, SB)
    above, below = slice(0, ROWS), slice(ROWS, 2 * ROWS)
    to_up[:, low] = (
        q1[:, low].astype(f32) + r[above, low].astype(f32) + near_low[...].astype(f32)
    ).astype(bf16)
    to_up[:, high] = (q1[:, high].astype(f32) + r[above, high].astype(f32)).astype(bf16)
    to_down[:, low] = (qm[:, low].astype(f32) + r[below, low].astype(f32)).astype(bf16)
    to_down[:, high] = (
        qm[:, high].astype(f32) + r[below, high].astype(f32) + near_high[...].astype(f32)
    ).astype(bf16)


def a_sum_kernel(own, below_low, above_low, below_high, above_high, mine, other):
    for cols, below, above in (
        (slice(0, SH), below_low, above_low),
        (slice(SH, SA), below_high, above_high),
    ):
        total = own[:, cols].astype(f32) + below[...].astype(f32) + above[...].astype(f32)
        mine[:, cols] = total[:ROWS, :]
        other[:, cols] = total[ROWS:, :].astype(bf16)


def gain_sum_kernel(mine, arrived, out):
    out[...] = mine[...] + arrived[...]


def token_kernel(
    tokens, gain, own_a, from_x, q0, r0, from_below, from_above, part, other_part, out, grad_gain
):
    grad_gain[...] = part[...] + other_part[...]
    wide = tokens[...].astype(f32)
    inverse = lax.rsqrt(jnp.mean(wide * wide, axis=-1, keepdims=True) + epsilon)
    hat = wide * inverse
    sum_a = own_a[...] + from_x[...].astype(f32)
    sum_b = (q0[...].astype(f32) + r0[...].astype(f32)) + (
        from_below[...].astype(f32) + from_above[...].astype(f32)
    )
    scaled_a = sum_a * gain[:, :SA]
    scaled_b = sum_b * gain[:, SA:]
    mean = (
        jnp.sum(scaled_a * hat[:, :SA], axis=-1, keepdims=True)
        + jnp.sum(scaled_b * hat[:, SA:], axis=-1, keepdims=True)
    ) / MODEL
    out[:, :SA] = (inverse * (scaled_a - hat[:, :SA] * mean)).astype(bf16)
    out[:, SA:] = (inverse * (scaled_b - hat[:, SA:] * mean)).astype(bf16)


def outer_kernel(mean_parts, fragment, momentum, new_fragment, new_momentum):
    count = mean_parts.shape[1]
    for j in range(mean_parts.shape[0]):
        rows = slice(j * count, (j + 1) * count)
        mean = mean_parts[j]
        change = outer_momentum * momentum[rows, :] + mean
        new_momentum[rows, :] = change
        new_fragment[rows, :] = fragment[rows, :] - outer_rate * (mean + outer_momentum * change)


def rope_tables(sequence_length, width):
    middle = width // 2
    frequency = rope_base ** (-2.0 * jnp.arange(middle, dtype=f32) / width)
    frequency = jnp.concatenate([frequency, frequency])
    angles = jnp.arange(sequence_length, dtype=f32)[:, None] * frequency[None, :]
    return jnp.cos(angles), jnp.sin(angles)


def swapped(bit):
    return [(index(x, y), index(x, y ^ bit)) for x in range(2) for y in range(4)]


def body(
    tokens,
    norm_gain,
    w_query,
    key_weight,
    value_weight,
    attention_gradient,
    global_fragment,
    momentum,
    local_fragment,
):
    rows = tokens[0]
    wq, wk, wv = w_query[0], key_weight[0], value_weight[0]
    me = lax.axis_index("tp")
    step_x = jnp.array([b[0] for b in BLOCKS], jnp.int32)
    step_y = jnp.array([b[1] for b in BLOCKS], jnp.int32)
    at = ((me // 4 + step_x) % 2) * 4 + (me % 4 + step_y + 4) % 4

    a00, b00 = call(
        norm_kernel, "norm", [shape(ROWS, A), shape(ROWS, B)], [rows, norm_gain], 10**6
    )
    a10 = across(a00)
    bm = up(b00)
    bp = down(b00)
    am = up(a00)
    ap = down(a00)
    b10 = across(b00)
    b2l = up(bm[:, :HB])
    b2h = down(bp[:, HB:])
    b1m = across(bm)
    b1p = across(bp)
    a1m = up(a10)
    a1p = down(a10)
    b12l = across(b2l)
    b12h = across(b2h)
    a02 = up(am)
    a12 = down(a1p)

    parts_a = [a00, a10, am, ap, a1m, a1p, a02, a12]
    parts_b = [b00, b10, bm, bp, b1m, b1p]
    halves = [b2l, b2h, b12l, b12h]
    weights = [wq, wk, wv]
    (first,) = call(
        functools.partial(project_kernel, 4, False),
        "project_first",
        [shape(512, 512, dtype=f32)],
        parts_a[:4] + parts_b[:4] + weights,
        2 * 512 * 512 * MODEL,
    )
    (second,) = call(
        functools.partial(project_kernel, 2, False),
        "project_second",
        [shape(256, 512, dtype=f32)],
        parts_a[4:6] + parts_b[4:6] + weights,
        2 * 256 * 512 * MODEL,
    )
    (third,) = call(
        functools.partial(project_kernel, 2, True),
        "project_third",
        [shape(256, 512, dtype=f32)],
        parts_a[6:] + halves + weights,
        2 * 256 * 512 * MODEL,
    )
    cosine, sine = rope_tables(SEQ, HEAD_SIZE)
    (grads,) = call(
        attention_kernel,
        "attention",
        [shape(SEQ, 512)],
        [at, first, second, third, cosine, sine, attention_gradient[0]],
        10 * SEQ * SEQ * 256,
        scratch=[
            pltpu.VMEM((SEQ, 256), bf16),
            pltpu.VMEM((SEQ, 128), bf16),
            pltpu.VMEM((SEQ, 128), bf16),
            pltpu.VMEM((SEQ, 128), f32),
            pltpu.VMEM((SEQ, 128), f32),
        ],
        smem=1,
    )
    far_low, far_high = call(
        far_back_kernel,
        "back_far",
        [shape(256, SH), shape(256, SA - SH)],
        [at, grads] + weights,
        2 * 512 * 256 * SA,
        smem=1,
    )
    x2, x1m, x0 = call(
        other_back_kernel,
        "back_other",
        [shape(ROWS, SB), shape(2 * ROWS, SB), shape(ROWS, SB)],
        [at, grads] + weights,
        2 * 512 * 512 * SB,
        smem=1,
    )
    near_low = up(far_low)
    near_high = down(far_high)
    r2 = across(x2)
    r1m = across(x1m)
    r0 = across(x0)
    up_low, up_high, down_low, down_high, own_a, q2, q1, qm, q0 = call(
        near_back_kernel,
        "back_near",
        [shape(256, SH), shape(256, SA - SH)] * 2 + [shape(256, SA)] + [shape(ROWS, SB)] * 4,
        [at, grads] + weights,
        2 * 512 * (768 * SA + 512 * SB),
        smem=1,
    )
    below_high = up(up_high)
    above_low = down(down_low)
    far_b_low, far_b_high = call(
        far_sum_kernel, "far_sum", [shape(ROWS, SHB), shape(ROWS, SB - SHB)], [q2, r2], 10**5
    )
    near_b_low = up(far_b_low)
    near_b_high = down(far_b_high)
    to_up, to_down = call(
        near_sum_kernel,
        "near_sum",
        [shape(256, SH), shape(256, SA - SH)],
        [up_low, near_low, down_high, near_high],
        10**5,
    )
    below_low = up(to_up)
    above_high = down(to_down)
    b_up, b_down = call(
        b_sum_kernel,
        "b_sum",
        [shape(ROWS, SB)] * 2,
        [q1, qm, r1m, near_b_low, near_b_high],
        10**5,
    )
    from_below = up(b_up)
    from_above = down(b_down)
    own_sum, other_sum_a = call(
        a_sum_kernel,
        "a_sum",
        [shape(ROWS, SA, dtype=f32), shape(ROWS, SA)],
        [own_a, below_low, above_low, below_high, above_high],
        10**5,
    )
    from_x = across(other_sum_a)

    grad_wq, grad_wk, grad_wv, gain_part = call(
        weight_kernel,
        "weights",
        [shape(MODEL, 256), shape(MODEL, 128), shape(MODEL, 128), shape(1, MODEL, dtype=f32)],
        [at] + parts_a + parts_b + halves + [grads] + weights + [norm_gain],
        2 * SEQ * 512 * MODEL,
        scratch=[pltpu.VMEM((SEQ, 512), bf16), pltpu.VMEM((256, B), bf16)],
        smem=1,
    )
    gain_row = [shape(1, MODEL, dtype=f32)]
    arrived_gain = lax.ppermute(gain_part, "tp", X_PAIRS)
    (gain_part,) = call(gain_sum_kernel, "e_sum0", gain_row, [gain_part, arrived_gain], 10**4)
    arrived_gain = lax.ppermute(gain_part, "tp", swapped(1))
    (gain_part,) = call(gain_sum_kernel, "e_sum1", gain_row, [gain_part, arrived_gain], 10**4)
    arrived_gain = lax.ppermute(gain_part, "tp", swapped(2))
    grad_rows, grad_gain = call(
        token_kernel,
        "tokens",
        [shape(ROWS, MODEL)] + gain_row,
        [rows, norm_gain, own_sum, from_x, q0, r0, from_below, from_above]
        + [gain_part, arrived_gain],
        10**6,
    )

    replicas = lax.axis_size("rep")
    near = replicas // 2
    groups = [list(range(near)), list(range(near, replicas))]
    count = global_fragment.shape[0] // near
    parts = local_fragment[0].reshape(near, count, MODEL)
    arrived = lax.all_to_all(
        parts, "rep", split_axis=0, concat_axis=0, tiled=True, axis_index_groups=groups
    )
    offset = lax.axis_index("rep") % near * count
    global_rows = lax.dynamic_slice_in_dim(global_fragment, offset, count, 0)
    half_sum = jnp.sum(global_rows[None] - arrived.astype(f32), axis=0)
    other_sum = lax.ppermute(half_sum, "rep", [(i, (i + near) % replicas) for i in range(replicas)])
    mean_rows = (half_sum + other_sum) / replicas
    copies = jnp.broadcast_to(mean_rows, (near, *mean_rows.shape))
    mean = lax.all_to_all(
        copies, "rep", split_axis=0, concat_axis=0, tiled=True, axis_index_groups=groups
    )
    new_global, new_momentum = call(
        outer_kernel,
        "outer",
        [shape(*momentum.shape, dtype=f32)] * 2,
        [mean, global_fragment, momentum],
        10**5,
    )
    return (
        grad_wq[None],
        grad_wk[None],
        grad_wv[None],
        grad_gain,
        grad_rows[None],
        new_global,
        new_momentum,
    )


def solution(mesh):
    placed = (
        P("rep", "tp", None),
        P("rep", None),
        P("rep", None, "tp"),
        P("rep", None, "tp"),
        P("rep", None, "tp"),
        P("rep", None, "tp"),
        P("tp", None),
        P("tp", None),
        P("rep", "tp", None),
    )

    return jax.shard_map(
        body,
        mesh=mesh,
        in_specs=placed,
        out_specs=(
            P("rep", None, "tp"),
            P("rep", None, "tp"),
            P("rep", None, "tp"),
            P("rep", None),
            P("rep", "tp", None),
            P("tp", None),
            P("tp", None),
        ),
        check_vma=False,
    )
```

```python
import functools

import jax
import jax.numpy as jnp
from jax import lax
from jax.experimental import pallas as pl
from jax.experimental.pallas import tpu as pltpu
from jax.sharding import PartitionSpec as P


HEAD_SIZE = 128
A = 1792
MODEL = 3072
B = MODEL - A
SA = 1536
SB = MODEL - SA
SH = 768
SHB = 768
ROWS = 128
SEQ = 1024
TILE = 256
STRIDE = 32
STEP_A = 896
STEP_B = 640

epsilon = 1e-05
rope_base = 500000.0
outer_rate = 0.7
outer_momentum = 0.9


f32 = jnp.float32
bf16 = jnp.bfloat16
NT = (((1,), (1,)), ((), ()))
TN = (((0,), (0,)), ((), ()))
NN = (((1,), (0,)), ((), ()))

BLOCKS = ((0, 0), (1, 0), (0, -1), (0, 1), (1, -1), (1, 1), (0, 2), (1, 2))
WHERE = {block: at for at, block in enumerate(BLOCKS)}


def index(x, y):
    return x * 4 + y % 4


X_PAIRS = [(index(x, y), index(1 - x, y)) for x in range(2) for y in range(4)]
UP_PAIRS = [(index(x, y), index(x, y + 1)) for x in range(2) for y in range(4)]
DOWN_PAIRS = [(index(x, y), index(x, y - 1)) for x in range(2) for y in range(4)]


def across(value):
    return lax.ppermute(value, "tp", X_PAIRS)


def up(value):
    return lax.ppermute(value, "tp", UP_PAIRS)


def down(value):
    return lax.ppermute(value, "tp", DOWN_PAIRS)


def dot(a, b, dims):
    return lax.dot_general(a, b, dims, preferred_element_type=f32)


VMEM_LIMIT = {"attention": 16, "weights": 16, "project_first": 16}
VM = pl.BlockSpec(memory_space=pltpu.VMEM)
SM = pl.BlockSpec(memory_space=pltpu.SMEM)


def call(kernel, name, outs, ins, flops, scratch=(), smem=0):
    nbytes = sum(v.size * v.dtype.itemsize for v in ins) + sum(
        o.size * o.dtype.itemsize for o in outs
    )
    return pl.pallas_call(
        kernel,
        out_shape=tuple(outs),
        in_specs=[SM] * smem + [VM] * (len(ins) - smem),
        out_specs=tuple([VM] * len(outs)),
        scratch_shapes=list(scratch),
        cost_estimate=pl.CostEstimate(flops=flops, bytes_accessed=nbytes, transcendentals=0),
        compiler_params=pltpu.CompilerParams(vmem_limit_bytes=VMEM_LIMIT.get(name, 8) * 1024 * 1024),
    )(*ins)


def shape(*dims, dtype=bf16):
    return jax.ShapeDtypeStruct(dims, dtype)


def norm_kernel(tokens, gain, part_a, part_b):
    wide = tokens[...].astype(f32)
    inverse = lax.rsqrt(jnp.mean(wide * wide, axis=-1, keepdims=True) + epsilon)
    part_a[...] = (wide[:, :A] * inverse * gain[:, :A]).astype(bf16)
    part_b[...] = (wide[:, A:] * inverse * gain[:, A:]).astype(bf16)


def project_kernel(n, *refs):
    wq, wk, wv, out = refs[2 * n :]
    rows_a = jnp.concatenate([r[...] for r in refs[:n]], axis=0)
    rows_b = jnp.concatenate([r[...] for r in refs[n : 2 * n]], axis=0)
    out[:, :256] = dot(rows_a, wq[:A, :], NN) + dot(rows_b, wq[A:, :], NN)
    both = jnp.concatenate([wk[...], wv[...]], axis=1)
    out[:, 256:] = dot(rows_a, both[:A, :], NN) + dot(rows_b, both[A:, :], NN)


def join_kernel(low, high, out):
    out[: ROWS // 2, :] = low[...]
    out[ROWS // 2 :, :] = high[...]


def share_kernel(local, out):
    count = out.shape[1]
    for j in range(out.shape[0]):
        out[j] = local[j * count : (j + 1) * count, :]


def spread_kernel(mine, other, out):
    mean = (mine[...] + other[...]) / (2 * out.shape[0])
    for j in range(out.shape[0]):
        out[j] = mean


def sign_row():
    lane = lax.broadcasted_iota(jnp.int32, (1, HEAD_SIZE), 1)
    return jnp.where(lane < HEAD_SIZE // 2, -1.0, 1.0).astype(f32)


def attention_kernel(
    at, first, second, third, coarse, fine, grad_out, out, qs, ks, vs, dk, dv, cosine, sine
):
    sign = sign_row()
    scale = HEAD_SIZE ** (-0.5)
    fine_cos, fine_sin = fine[:STRIDE, :], fine[STRIDE:, :]
    for a in range(SEQ // STRIDE):
        c, s = coarse[a : a + 1, :], coarse[SEQ // STRIDE + a : SEQ // STRIDE + a + 1, :]
        cosine[a * STRIDE : (a + 1) * STRIDE, :] = c * fine_cos - s * fine_sin
        sine[a * STRIDE : (a + 1) * STRIDE, :] = s * fine_cos + c * fine_sin

    def rotate(v, c, s):
        return v * c + pltpu.roll(v, HEAD_SIZE // 2, 1) * (sign * s)

    def rotate_back(g, c, s):
        return g * c - pltpu.roll(g * s, HEAD_SIZE // 2, 1) * sign

    def place(source, base, j):
        here = pl.ds(pl.multiple_of(at[j] * ROWS, ROWS), ROWS)
        c, s = cosine[here, :], sine[here, :]
        block = source[pl.ds(pl.multiple_of(base, ROWS), ROWS), :]
        qs[here, :128] = rotate(block[:, :128], c, s).astype(bf16)
        qs[here, 128:] = rotate(block[:, 128:256], c, s).astype(bf16)
        ks[here, :] = rotate(block[:, 256:384], c, s).astype(bf16)
        vs[here, :] = block[:, 384:].astype(bf16)

    @pl.loop(0, 4)
    def _(j):
        place(first, j * ROWS, j)

    @pl.loop(0, 2)
    def _(j):
        place(second, j * ROWS, j + 4)
        place(third, j * ROWS, j + 6)

    dk[...] = jnp.zeros_like(dk)
    dv[...] = jnp.zeros_like(dv)
    key_at = lax.broadcasted_iota(jnp.int32, (TILE, TILE), 0)
    query_at = lax.broadcasted_iota(jnp.int32, (TILE, TILE), 1)
    allowed = key_at <= query_at
    for i in range(SEQ // TILE):
        lo, hi = i * TILE, (i + 1) * TILE

        keys, values = ks[:hi, :], vs[:hi, :]
        for h in range(2):
            cols = slice(h * 128, (h + 1) * 128)
            q, g = qs[lo:hi, cols], grad_out[lo:hi, cols]
            scores = dot(keys, q, NT) * scale
            last = jnp.where(allowed, scores[lo:, :], -jnp.inf)
            scores = jnp.concatenate([scores[:lo, :], last], axis=0) if i else last
            powers = jnp.exp(scores - jnp.max(scores, axis=0, keepdims=True))
            probability = powers * (1.0 / jnp.sum(powers, axis=0, keepdims=True))
            dv[:hi, :] += dot(probability.astype(bf16), g, NN)
            grad_prob = dot(values, g, NT)
            row = jnp.sum(grad_prob * probability, axis=0, keepdims=True)
            grad_score = (probability * (grad_prob - row) * scale).astype(bf16)
            dk[:hi, :] += dot(grad_score, q, NN)
            dq = dot(grad_score, keys, TN)
            out[lo:hi, cols] = rotate_back(dq, cosine[lo:hi, :], sine[lo:hi, :]).astype(bf16)

    out[:, 256:384] = rotate_back(dk[...], cosine[...], sine[...]).astype(bf16)
    out[:, 384:] = dv[...].astype(bf16)


def rows_of(at, ref, block):
    return ref[pl.ds(pl.multiple_of(at[WHERE[block]] * ROWS, ROWS), ROWS), :]


def back_tile(rows, wq, wk, wv, cols):
    both = jnp.concatenate([wk[cols, :], wv[cols, :]], axis=1)
    return (dot(rows[:, :256], wq[cols, :], NT) + dot(rows[:, 256:], both, NT)).astype(bf16)


def columns(i, base=0):
    return pl.ds(pl.multiple_of(i * TILE + base, TILE), TILE)


def far_back_kernel(at, grads, wq, wk, wv, far_low, far_high):
    far = jnp.concatenate([rows_of(at, grads, (0, 2)), rows_of(at, grads, (1, 2))], axis=0)

    @pl.loop(0, SH // TILE)
    def _(i):
        far_low[:, columns(i)] = back_tile(far, wq, wk, wv, columns(i))
        far_high[:, columns(i)] = back_tile(far, wq, wk, wv, columns(i, SH))


def other_back_kernel(at, grads, wq, wk, wv, x2, x1m, x0):
    other = jnp.concatenate([rows_of(at, grads, (1, d)) for d in (2, 1, -1, 0)], axis=0)

    @pl.loop(0, SHB // TILE)
    def _(i):
        for base in (0, SHB):
            tile = back_tile(other, wq, wk, wv, columns(i, SA + base))
            x2[:, columns(i, base)] = tile[:ROWS, :]
            x1m[:, columns(i, base)] = tile[ROWS : 3 * ROWS, :]
            x0[:, columns(i, base)] = tile[3 * ROWS :, :]


def near_back_kernel(
    at, grads, wq, wk, wv, up_low, up_high, down_low, down_high, own_a, q2, q1, qm, q0
):
    near = jnp.concatenate(
        [rows_of(at, grads, (x, d)) for d in (1, -1, 0) for x in (0, 1)], axis=0
    )
    mine = jnp.concatenate([rows_of(at, grads, (0, d)) for d in (2, 1, -1, 0)], axis=0)

    @pl.loop(0, SH // TILE)
    def _(i):
        for base, above, below in ((0, up_low, down_low), (SH, up_high, down_high)):
            tile = back_tile(near, wq, wk, wv, columns(i, base))
            above[:, columns(i)] = tile[:256, :]
            below[:, columns(i)] = tile[256:512, :]
            own_a[:, columns(i, base)] = tile[512:, :]

    @pl.loop(0, SHB // TILE)
    def _(i):
        for base in (0, SHB):
            tile = back_tile(mine, wq, wk, wv, columns(i, SA + base))
            for n, ref in enumerate((q2, q1, qm, q0)):
                ref[:, columns(i, base)] = tile[n * ROWS : (n + 1) * ROWS, :]


def weight_kernel(at, *refs):
    parts_a, parts_b = refs[:8], refs[8:16]
    grads, wq, wk, wv, gain, dwq, dwk, dwv, gain_part, ordered = refs[16:]
    for j in range(8):
        ordered[j * ROWS : (j + 1) * ROWS, :] = grads[
            pl.ds(pl.multiple_of(at[j] * ROWS, ROWS), ROWS), :
        ]

    def tile(rows, to, size):
        product = dot(rows, ordered[...], TN)
        where = pl.ds(to, size)
        dwq[where, :] = product[:, :256].astype(bf16)
        dwk[where, :] = product[:, 256:384].astype(bf16)
        dwv[where, :] = product[:, 384:].astype(bf16)
        total = (
            product[:, :128] * wq[where, :128].astype(f32)
            + product[:, 128:256] * wq[where, 128:].astype(f32)
            + product[:, 256:384] * wk[where, :].astype(f32)
            + product[:, 384:] * wv[where, :].astype(f32)
        )
        gain_part[:, where] = jnp.sum(total.T, axis=0, keepdims=True) / gain[:, where]

    @pl.loop(0, A // STEP_A)
    def _(i):
        col = pl.multiple_of(i * STEP_A, 128)
        rows = [r[:, pl.ds(col, STEP_A)] for r in parts_a]
        tile(jnp.concatenate(rows, axis=0), col, STEP_A)

    @pl.loop(0, B // STEP_B)
    def _(i):
        col = pl.multiple_of(i * STEP_B, 128)
        rows = [r[:, pl.ds(col, STEP_B)] for r in parts_b]
        tile(jnp.concatenate(rows, axis=0), pl.multiple_of(A + col, 128), STEP_B)


def near_sum_kernel(up_low, near_low, down_high, near_high, mine, arrived, to_up, to_down):
    count = 2 * ROWS
    to_up[:count, :] = (up_low[...].astype(f32) + near_low[...].astype(f32)).astype(bf16)
    to_down[:count, :] = (down_high[...].astype(f32) + near_high[...].astype(f32)).astype(bf16)
    total = (mine[...].astype(f32) + arrived[...].astype(f32)).astype(bf16)
    to_up[count:, :] = total[:, :SHB]
    to_down[count:, :] = total[:, SHB:]


def b_sum_kernel(q1, qm, r, near_low, near_high, to_up, to_down):
    low, high = slice(0, SHB), slice(SHB, SB)
    above, below = slice(0, ROWS), slice(ROWS, 2 * ROWS)
    to_up[:, low] = (
        q1[:, low].astype(f32) + r[above, low].astype(f32) + near_low[2 * ROWS :, :].astype(f32)
    ).astype(bf16)
    to_up[:, high] = (q1[:, high].astype(f32) + r[above, high].astype(f32)).astype(bf16)
    to_down[:, low] = (qm[:, low].astype(f32) + r[below, low].astype(f32)).astype(bf16)
    to_down[:, high] = (
        qm[:, high].astype(f32) + r[below, high].astype(f32) + near_high[2 * ROWS :, :].astype(f32)
    ).astype(bf16)


def a_sum_kernel(own, below_low, above_low, below_high, above_high, mine, other):
    count = 2 * ROWS
    for cols, below, above in (
        (slice(0, SH), below_low[:count, :], above_low[...]),
        (slice(SH, SA), below_high[...], above_high[:count, :]),
    ):
        total = own[:, cols].astype(f32) + below.astype(f32) + above.astype(f32)
        mine[:, cols] = total[:ROWS, :]
        other[:, cols] = total[ROWS:, :].astype(bf16)


def gain_sum_kernel(mine, arrived, out):
    out[...] = mine[...] + arrived[...]


def token_kernel(
    tokens, gain, own_a, from_x, q0, r0, from_below, from_above, out
):
    wide = tokens[...].astype(f32)
    inverse = lax.rsqrt(jnp.mean(wide * wide, axis=-1, keepdims=True) + epsilon)
    hat = wide * inverse
    sum_a = own_a[...] + from_x[...].astype(f32)
    sum_b = (q0[...].astype(f32) + r0[...].astype(f32)) + (
        from_below[...].astype(f32) + from_above[...].astype(f32)
    )
    scaled_a = sum_a * gain[:, :SA]
    scaled_b = sum_b * gain[:, SA:]
    mean = (
        jnp.sum(scaled_a * hat[:, :SA], axis=-1, keepdims=True)
        + jnp.sum(scaled_b * hat[:, SA:], axis=-1, keepdims=True)
    ) / MODEL
    out[:, :SA] = (inverse * (scaled_a - hat[:, :SA] * mean)).astype(bf16)
    out[:, SA:] = (inverse * (scaled_b - hat[:, SA:] * mean)).astype(bf16)


def outer_kernel(
    mean_parts, fragment, momentum, part, other_part, new_fragment, new_momentum, grad_gain
):
    grad_gain[...] = part[...] + other_part[...]
    count = mean_parts.shape[1]

    @pl.loop(0, mean_parts.shape[0] // 2)
    def _(i):
        rows = pl.ds(pl.multiple_of(i * 2 * count, 2 * count), 2 * count)
        mean = jnp.concatenate([mean_parts[2 * i], mean_parts[2 * i + 1]], axis=0)
        change = outer_momentum * momentum[rows, :] + mean
        new_momentum[rows, :] = change
        new_fragment[rows, :] = fragment[rows, :] - outer_rate * (mean + outer_momentum * change)


def rope_tables(positions, width):
    middle = width // 2
    frequency = rope_base ** (-2.0 * jnp.arange(middle, dtype=f32) / width)
    frequency = jnp.concatenate([frequency, frequency])
    angles = positions.astype(f32)[:, None] * frequency[None, :]
    return jnp.concatenate([jnp.cos(angles), jnp.sin(angles)], axis=0)


def swapped(bit):
    return [(index(x, y), index(x, y ^ bit)) for x in range(2) for y in range(4)]


def body(
    tokens,
    norm_gain,
    w_query,
    key_weight,
    value_weight,
    attention_gradient,
    global_fragment,
    momentum,
    local_fragment,
):
    rows = tokens[0]
    wq, wk, wv = w_query[0], key_weight[0], value_weight[0]
    me = lax.axis_index("tp")
    step_x = jnp.array([b[0] for b in BLOCKS], jnp.int32)
    step_y = jnp.array([b[1] for b in BLOCKS], jnp.int32)
    at = ((me // 4 + step_x) % 2) * 4 + (me % 4 + step_y + 4) % 4

    a00, b00 = call(
        norm_kernel, "norm", [shape(ROWS, A), shape(ROWS, B)], [rows, norm_gain], 10**6
    )
    a10 = across(a00)
    bm = up(b00)
    bp = down(b00)
    am = up(a00)
    ap = down(a00)
    b10 = across(b00)
    half = ROWS // 2
    b2l = up(bm[:half])
    b2h = down(bp[half:])
    (b2,) = call(join_kernel, "join", [shape(ROWS, B)], [b2l, b2h], 10**4)
    b1m = across(bm)
    b1p = across(bp)
    a1m = up(a10)
    a1p = down(a10)
    b12 = across(b2)
    a02 = up(am)
    a12 = down(a1p)

    parts_a = [a00, a10, am, ap, a1m, a1p, a02, a12]
    parts_b = [b00, b10, bm, bp, b1m, b1p, b2, b12]
    weights = [wq, wk, wv]
    (first,) = call(
        functools.partial(project_kernel, 4),
        "project_first",
        [shape(512, 512, dtype=f32)],
        parts_a[:4] + parts_b[:4] + weights,
        2 * 512 * 512 * MODEL,
    )
    (second,) = call(
        functools.partial(project_kernel, 2),
        "project_second",
        [shape(256, 512, dtype=f32)],
        parts_a[4:6] + parts_b[4:6] + weights,
        2 * 256 * 512 * MODEL,
    )
    (third,) = call(
        functools.partial(project_kernel, 2),
        "project_third",
        [shape(256, 512, dtype=f32)],
        parts_a[6:] + parts_b[6:] + weights,
        2 * 256 * 512 * MODEL,
    )
    coarse = rope_tables(jnp.arange(0, SEQ, STRIDE), HEAD_SIZE)
    fine = rope_tables(jnp.arange(STRIDE), HEAD_SIZE)
    (grads,) = call(
        attention_kernel,
        "attention",
        [shape(SEQ, 512)],
        [at, first, second, third, coarse, fine, attention_gradient[0]],
        10 * SEQ * SEQ * 256,
        scratch=[
            pltpu.VMEM((SEQ, 256), bf16),
            pltpu.VMEM((SEQ, 128), bf16),
            pltpu.VMEM((SEQ, 128), bf16),
        ]
        + [pltpu.VMEM((SEQ, 128), f32)] * 4,
        smem=1,
    )
    far_low, far_high = call(
        far_back_kernel,
        "back_far",
        [shape(256, SH), shape(256, SA - SH)],
        [at, grads] + weights,
        2 * 512 * 256 * SA,
        smem=1,
    )
    x2, x1m, x0 = call(
        other_back_kernel,
        "back_other",
        [shape(ROWS, SB), shape(2 * ROWS, SB), shape(ROWS, SB)],
        [at, grads] + weights,
        2 * 512 * 512 * SB,
        smem=1,
    )
    near_low = up(far_low)
    near_high = down(far_high)
    r2 = across(x2)
    r1m = across(x1m)
    r0 = across(x0)
    up_low, up_high, down_low, down_high, own_a, q2, q1, qm, q0 = call(
        near_back_kernel,
        "back_near",
        [shape(256, SH), shape(256, SA - SH)] * 2 + [shape(256, SA)] + [shape(ROWS, SB)] * 4,
        [at, grads] + weights,
        2 * 512 * (768 * SA + 512 * SB),
        smem=1,
    )
    below_high = up(up_high)
    above_low = down(down_low)
    to_up, to_down = call(
        near_sum_kernel,
        "near_sum",
        [shape(3 * ROWS, SH)] * 2,
        [up_low, near_low, down_high, near_high, q2, r2],
        10**5,
    )
    below_low = up(to_up)
    above_high = down(to_down)
    b_up, b_down = call(
        b_sum_kernel,
        "b_sum",
        [shape(ROWS, SB)] * 2,
        [q1, qm, r1m, below_low, above_high],
        10**5,
    )
    from_below = up(b_up)
    from_above = down(b_down)
    own_sum, other_sum_a = call(
        a_sum_kernel,
        "a_sum",
        [shape(ROWS, SA, dtype=f32), shape(ROWS, SA)],
        [own_a, below_low, above_low, below_high, above_high],
        10**5,
    )
    from_x = across(other_sum_a)

    grad_wq, grad_wk, grad_wv, gain_part = call(
        weight_kernel,
        "weights",
        [shape(MODEL, 256), shape(MODEL, 128), shape(MODEL, 128), shape(1, MODEL, dtype=f32)],
        [at] + parts_a + parts_b + [grads] + weights + [norm_gain],
        2 * SEQ * 512 * MODEL,
        scratch=[pltpu.VMEM((SEQ, 512), bf16)],
        smem=1,
    )
    gain_row = [shape(1, MODEL, dtype=f32)]
    arrived_gain = lax.ppermute(gain_part, "tp", X_PAIRS)
    (gain_part,) = call(gain_sum_kernel, "e_sum0", gain_row, [gain_part, arrived_gain], 10**4)
    arrived_gain = lax.ppermute(gain_part, "tp", swapped(1))
    (gain_part,) = call(gain_sum_kernel, "e_sum1", gain_row, [gain_part, arrived_gain], 10**4)
    arrived_gain = lax.ppermute(gain_part, "tp", swapped(2))
    (grad_rows,) = call(
        token_kernel,
        "tokens",
        [shape(ROWS, MODEL)],
        [rows, norm_gain, own_sum, from_x, q0, r0, from_below, from_above],
        10**6,
    )

    replicas = lax.axis_size("rep")
    near = replicas // 2
    groups = [list(range(near)), list(range(near, replicas))]
    count = global_fragment.shape[0] // near
    (parts,) = call(
        share_kernel, "share", [shape(near, count, MODEL)], [local_fragment[0]], 10**4
    )
    arrived = lax.all_to_all(
        parts, "rep", split_axis=0, concat_axis=0, tiled=True, axis_index_groups=groups
    )
    offset = lax.axis_index("rep") % near * count
    global_rows = lax.dynamic_slice_in_dim(global_fragment, offset, count, 0)
    half_sum = jnp.sum(global_rows[None] - arrived.astype(f32), axis=0)
    other_sum = lax.ppermute(half_sum, "rep", [(i, (i + near) % replicas) for i in range(replicas)])
    (copies,) = call(
        spread_kernel, "spread", [shape(near, count, MODEL, dtype=f32)], [half_sum, other_sum], 10**4
    )
    mean = lax.all_to_all(
        copies, "rep", split_axis=0, concat_axis=0, tiled=True, axis_index_groups=groups
    )
    new_global, new_momentum, grad_gain = call(
        outer_kernel,
        "outer",
        [shape(*momentum.shape, dtype=f32)] * 2 + gain_row,
        [mean, global_fragment, momentum, gain_part, arrived_gain],
        10**5,
    )
    return (
        grad_wq[None],
        grad_wk[None],
        grad_wv[None],
        grad_gain,
        grad_rows[None],
        new_global,
        new_momentum,
    )


def solution(mesh):
    placed = (
        P("rep", "tp", None),
        P("rep", None),
        P("rep", None, "tp"),
        P("rep", None, "tp"),
        P("rep", None, "tp"),
        P("rep", None, "tp"),
        P("tp", None),
        P("tp", None),
        P("rep", "tp", None),
    )

    return jax.shard_map(
        body,
        mesh=mesh,
        in_specs=placed,
        out_specs=(
            P("rep", None, "tp"),
            P("rep", None, "tp"),
            P("rep", None, "tp"),
            P("rep", None),
            P("rep", "tp", None),
            P("tp", None),
            P("tp", None),
        ),
        check_vma=False,
    )
```

```python
import functools

import jax
import jax.numpy as jnp
from jax import lax
from jax.experimental import pallas as pl
from jax.experimental.pallas import tpu as pltpu
from jax.sharding import PartitionSpec as P


HEAD_SIZE = 128
A = 1792
MODEL = 3072
B = MODEL - A
SA = 1536
SB = MODEL - SA
SH = 768
SHB = 768
ROWS = 128
SEQ = 1024
TILE = 256
STRIDE = 32
STEP_A = 896
STEP_B = 640

epsilon = 1e-05
rope_base = 500000.0
outer_rate = 0.7
outer_momentum = 0.9


f32 = jnp.float32
bf16 = jnp.bfloat16
NT = (((1,), (1,)), ((), ()))
TN = (((0,), (0,)), ((), ()))
NN = (((1,), (0,)), ((), ()))

BLOCKS = ((0, 0), (1, 0), (0, -1), (0, 1), (1, -1), (1, 1), (0, 2), (1, 2))
WHERE = {block: at for at, block in enumerate(BLOCKS)}


def index(x, y):
    return x * 4 + y % 4


X_PAIRS = [(index(x, y), index(1 - x, y)) for x in range(2) for y in range(4)]
UP_PAIRS = [(index(x, y), index(x, y + 1)) for x in range(2) for y in range(4)]
DOWN_PAIRS = [(index(x, y), index(x, y - 1)) for x in range(2) for y in range(4)]


def across(value):
    return lax.ppermute(value, "tp", X_PAIRS)


def up(value):
    return lax.ppermute(value, "tp", UP_PAIRS)


def down(value):
    return lax.ppermute(value, "tp", DOWN_PAIRS)


def dot(a, b, dims):
    return lax.dot_general(a, b, dims, preferred_element_type=f32)


VMEM_LIMIT = {"attention": 16, "weights": 16, "project_first": 16}
VM = pl.BlockSpec(memory_space=pltpu.VMEM)
SM = pl.BlockSpec(memory_space=pltpu.SMEM)


def call(kernel, name, outs, ins, flops, scratch=(), smem=0):
    nbytes = sum(v.size * v.dtype.itemsize for v in ins) + sum(
        o.size * o.dtype.itemsize for o in outs
    )
    return pl.pallas_call(
        kernel,
        out_shape=tuple(outs),
        in_specs=[SM] * smem + [VM] * (len(ins) - smem),
        out_specs=tuple([VM] * len(outs)),
        scratch_shapes=list(scratch),
        cost_estimate=pl.CostEstimate(flops=flops, bytes_accessed=nbytes, transcendentals=0),
        compiler_params=pltpu.CompilerParams(vmem_limit_bytes=VMEM_LIMIT.get(name, 8) * 1024 * 1024),
    )(*ins)


def shape(*dims, dtype=bf16):
    return jax.ShapeDtypeStruct(dims, dtype)


def each_block(count, body):
    size = 32

    @pl.loop(0, count // size)
    def _(i):
        body(pl.ds(pl.multiple_of(i * size, size), size))


def norm_kernel(tokens, gain, part_a, part_b):
    def body(at):
        wide = tokens[at, :].astype(f32)
        inverse = lax.rsqrt(jnp.mean(wide * wide, axis=-1, keepdims=True) + epsilon)
        part_a[at, :] = (wide[:, :A] * inverse * gain[:, :A]).astype(bf16)
        part_b[at, :] = (wide[:, A:] * inverse * gain[:, A:]).astype(bf16)

    each_block(ROWS, body)


def project_kernel(n, *refs):
    wq, wk, wv, out = refs[-4:]
    rows_a = jnp.concatenate([r[...] for r in refs[:n]], axis=0)
    rows_b = jnp.concatenate([r[...] for r in refs[n:-4]], axis=0)
    out[:, :256] = dot(rows_a, wq[:A, :], NN) + dot(rows_b, wq[A:, :], NN)
    both = jnp.concatenate([wk[...], wv[...]], axis=1)
    out[:, 256:] = dot(rows_a, both[:A, :], NN) + dot(rows_b, both[A:, :], NN)


def join_kernel(low, high, out):
    out[: low.shape[0], :] = low[...]
    out[low.shape[0] :, :] = high[...]


def share_kernel(local, out):
    count = out.shape[1]
    for j in range(out.shape[0]):
        out[j] = local[j * count : (j + 1) * count, :]


def spread_kernel(mine, other, out):
    mean = (mine[...] + other[...]) / (2 * out.shape[0])
    for j in range(out.shape[0]):
        out[j] = mean


def sign_row():
    lane = lax.broadcasted_iota(jnp.int32, (1, HEAD_SIZE), 1)
    return jnp.where(lane < HEAD_SIZE // 2, -1.0, 1.0).astype(f32)


def attention_kernel(
    at, first, second, third, coarse, fine, grad_out, out, qs, ks, vs, dk, dv, cosine, sine
):
    sign = sign_row()
    scale = HEAD_SIZE ** (-0.5)
    fine_cos, fine_sin = fine[:STRIDE, :], fine[STRIDE:, :]
    for a in range(SEQ // STRIDE):
        c, s = coarse[a : a + 1, :], coarse[SEQ // STRIDE + a : SEQ // STRIDE + a + 1, :]
        cosine[a * STRIDE : (a + 1) * STRIDE, :] = c * fine_cos - s * fine_sin
        sine[a * STRIDE : (a + 1) * STRIDE, :] = s * fine_cos + c * fine_sin

    def rotate(v, c, s):
        return v * c + pltpu.roll(v, HEAD_SIZE // 2, 1) * (sign * s)

    def rotate_back(g, c, s):
        return g * c - pltpu.roll(g * s, HEAD_SIZE // 2, 1) * sign

    def place(source, base, j):
        here = pl.ds(pl.multiple_of(at[j] * ROWS, ROWS), ROWS)
        c, s = cosine[here, :], sine[here, :]
        block = source[pl.ds(pl.multiple_of(base, ROWS), ROWS), :]
        qs[here, :128] = rotate(block[:, :128], c, s).astype(bf16)
        qs[here, 128:] = rotate(block[:, 128:256], c, s).astype(bf16)
        ks[here, :] = rotate(block[:, 256:384], c, s).astype(bf16)
        vs[here, :] = block[:, 384:].astype(bf16)

    @pl.loop(0, 4)
    def _(j):
        place(first, j * ROWS, j)

    @pl.loop(0, 2)
    def _(j):
        place(second, j * ROWS, j + 4)
        place(third, j * ROWS, j + 6)

    dk[...] = jnp.zeros_like(dk)
    dv[...] = jnp.zeros_like(dv)
    key_at = lax.broadcasted_iota(jnp.int32, (TILE, TILE), 0)
    query_at = lax.broadcasted_iota(jnp.int32, (TILE, TILE), 1)
    allowed = key_at <= query_at
    for i in range(SEQ // TILE):
        lo, hi = i * TILE, (i + 1) * TILE

        keys, values = ks[:hi, :], vs[:hi, :]
        for h in range(2):
            cols = slice(h * 128, (h + 1) * 128)
            q, g = qs[lo:hi, cols], grad_out[lo:hi, cols]
            scores = dot(keys, q, NT) * scale
            last = jnp.where(allowed, scores[lo:, :], -jnp.inf)
            scores = jnp.concatenate([scores[:lo, :], last], axis=0) if i else last
            powers = jnp.exp(scores - jnp.max(scores, axis=0, keepdims=True))
            probability = powers * (1.0 / jnp.sum(powers, axis=0, keepdims=True))
            dv[:hi, :] += dot(probability.astype(bf16), g, NN)
            grad_prob = dot(values, g, NT)
            row = jnp.sum(grad_prob * probability, axis=0, keepdims=True)
            grad_score = (probability * (grad_prob - row) * scale).astype(bf16)
            dk[:hi, :] += dot(grad_score, q, NN)
            dq = dot(grad_score, keys, TN)
            out[lo:hi, cols] = rotate_back(dq, cosine[lo:hi, :], sine[lo:hi, :]).astype(bf16)

    out[:, 256:384] = rotate_back(dk[...], cosine[...], sine[...]).astype(bf16)
    out[:, 384:] = dv[...].astype(bf16)


def rows_of(at, ref, block):
    return ref[pl.ds(pl.multiple_of(at[WHERE[block]] * ROWS, ROWS), ROWS), :]


def back_tile(rows, wq, wk, wv, cols):
    both = jnp.concatenate([wk[cols, :], wv[cols, :]], axis=1)
    return (dot(rows[:, :256], wq[cols, :], NT) + dot(rows[:, 256:], both, NT)).astype(bf16)


def columns(i, base=0):
    return pl.ds(pl.multiple_of(i * TILE + base, TILE), TILE)


def far_back_kernel(at, grads, wq, wk, wv, far_low, far_high):
    far = jnp.concatenate([rows_of(at, grads, (0, 2)), rows_of(at, grads, (1, 2))], axis=0)

    @pl.loop(0, SH // TILE)
    def _(i):
        far_low[:, columns(i)] = back_tile(far, wq, wk, wv, columns(i))
        far_high[:, columns(i)] = back_tile(far, wq, wk, wv, columns(i, SH))


def other_back_kernel(at, grads, wq, wk, wv, x2, x1m, x0):
    other = jnp.concatenate([rows_of(at, grads, (1, d)) for d in (2, 1, -1, 0)], axis=0)

    @pl.loop(0, SHB // TILE)
    def _(i):
        for base in (0, SHB):
            tile = back_tile(other, wq, wk, wv, columns(i, SA + base))
            x2[:, columns(i, base)] = tile[:ROWS, :]
            x1m[:, columns(i, base)] = tile[ROWS : 3 * ROWS, :]
            x0[:, columns(i, base)] = tile[3 * ROWS :, :]


def near_back_kernel(
    at, grads, wq, wk, wv, up_low, up_high, down_low, down_high, own_a, q2, q1, qm, q0
):
    near = jnp.concatenate(
        [rows_of(at, grads, (x, d)) for d in (1, -1, 0) for x in (0, 1)], axis=0
    )
    mine = jnp.concatenate([rows_of(at, grads, (0, d)) for d in (2, 1, -1, 0)], axis=0)

    @pl.loop(0, SH // TILE)
    def _(i):
        for base, above, below in ((0, up_low, down_low), (SH, up_high, down_high)):
            tile = back_tile(near, wq, wk, wv, columns(i, base))
            above[:, columns(i)] = tile[:256, :]
            below[:, columns(i)] = tile[256:512, :]
            own_a[:, columns(i, base)] = tile[512:, :]

    @pl.loop(0, SHB // TILE)
    def _(i):
        for base in (0, SHB):
            tile = back_tile(mine, wq, wk, wv, columns(i, SA + base))
            for n, ref in enumerate((q2, q1, qm, q0)):
                ref[:, columns(i, base)] = tile[n * ROWS : (n + 1) * ROWS, :]


def weight_kernel(at, *refs):
    parts_a, parts_b = refs[:8], refs[8:15]
    grads, wq, wk, wv, gain, dwq, dwk, dwv, gain_part, ordered = refs[15:]
    for j in range(8):
        ordered[j * ROWS : (j + 1) * ROWS, :] = grads[
            pl.ds(pl.multiple_of(at[j] * ROWS, ROWS), ROWS), :
        ]

    def tile(rows, to, size):
        product = dot(rows, ordered[...], TN)
        where = pl.ds(to, size)
        dwq[where, :] = product[:, :256].astype(bf16)
        dwk[where, :] = product[:, 256:384].astype(bf16)
        dwv[where, :] = product[:, 384:].astype(bf16)
        total = (
            product[:, :128] * wq[where, :128].astype(f32)
            + product[:, 128:256] * wq[where, 128:].astype(f32)
            + product[:, 256:384] * wk[where, :].astype(f32)
            + product[:, 384:] * wv[where, :].astype(f32)
        )
        gain_part[:, where] = jnp.sum(total.T, axis=0, keepdims=True) / gain[:, where]

    @pl.loop(0, A // STEP_A)
    def _(i):
        col = pl.multiple_of(i * STEP_A, 128)
        rows = [r[:, pl.ds(col, STEP_A)] for r in parts_a]
        tile(jnp.concatenate(rows, axis=0), col, STEP_A)

    @pl.loop(0, B // STEP_B)
    def _(i):
        col = pl.multiple_of(i * STEP_B, 128)
        rows = [r[:, pl.ds(col, STEP_B)] for r in parts_b]
        tile(jnp.concatenate(rows, axis=0), pl.multiple_of(A + col, 128), STEP_B)


def near_sum_kernel(up_low, near_low, down_high, near_high, mine, arrived, to_up, to_down):
    count = 2 * ROWS
    to_up[:count, :] = (up_low[...].astype(f32) + near_low[...].astype(f32)).astype(bf16)
    to_down[:count, :] = (down_high[...].astype(f32) + near_high[...].astype(f32)).astype(bf16)
    total = (mine[...].astype(f32) + arrived[...].astype(f32)).astype(bf16)
    to_up[count:, :] = total[:, :SHB]
    to_down[count:, :] = total[:, SHB:]


def b_sum_kernel(q1, qm, r, near_low, near_high, to_up, to_down):
    low, high = slice(0, SHB), slice(SHB, SB)
    size = 32

    @pl.loop(0, ROWS // size)
    def _(i):
        at = pl.ds(pl.multiple_of(i * size, size), size)
        below = pl.ds(pl.multiple_of(i * size + ROWS, size), size)
        near = pl.ds(pl.multiple_of(i * size + 2 * ROWS, size), size)

        def total(q, rows, cols):
            return q[at, cols].astype(f32) + r[rows, cols].astype(f32)

        to_up[at, low] = (total(q1, at, low) + near_low[near, :].astype(f32)).astype(bf16)
        to_up[at, high] = total(q1, at, high).astype(bf16)
        to_down[at, low] = total(qm, below, low).astype(bf16)
        to_down[at, high] = (total(qm, below, high) + near_high[near, :].astype(f32)).astype(bf16)


def a_sum_kernel(own, below_low, above_low, below_high, above_high, mine, other):
    size = 32

    @pl.loop(0, ROWS // size)
    def _(i):
        at = pl.ds(pl.multiple_of(i * size, size), size)
        far = pl.ds(pl.multiple_of(i * size + ROWS, size), size)
        for cols, below, above in (
            (slice(0, SH), below_low, above_low),
            (slice(SH, SA), below_high, above_high),
        ):

            def total(rows):
                return (
                    own[rows, cols].astype(f32)
                    + below[rows, :].astype(f32)
                    + above[rows, :].astype(f32)
                )

            mine[at, cols] = total(at)
            other[at, cols] = total(far).astype(bf16)


def gain_sum_kernel(mine, arrived, out):
    out[...] = mine[...] + arrived[...]


def token_kernel(tokens, gain, own_a, from_x, q0, r0, from_below, from_above, out):
    def body(at):
        wide = tokens[at, :].astype(f32)
        inverse = lax.rsqrt(jnp.mean(wide * wide, axis=-1, keepdims=True) + epsilon)
        hat = wide * inverse
        sum_a = own_a[at, :] + from_x[at, :].astype(f32)
        sum_b = (q0[at, :].astype(f32) + r0[at, :].astype(f32)) + (
            from_below[at, :].astype(f32) + from_above[at, :].astype(f32)
        )
        scaled_a = sum_a * gain[:, :SA]
        scaled_b = sum_b * gain[:, SA:]
        mean = (
            jnp.sum(scaled_a * hat[:, :SA], axis=-1, keepdims=True)
            + jnp.sum(scaled_b * hat[:, SA:], axis=-1, keepdims=True)
        ) / MODEL
        out[at, :SA] = (inverse * (scaled_a - hat[:, :SA] * mean)).astype(bf16)
        out[at, SA:] = (inverse * (scaled_b - hat[:, SA:] * mean)).astype(bf16)

    each_block(ROWS, body)


def outer_kernel(
    mean_parts, fragment, momentum, part, other_part, new_fragment, new_momentum, grad_gain
):
    grad_gain[...] = part[...] + other_part[...]
    count = mean_parts.shape[1]

    @pl.loop(0, mean_parts.shape[0] // 2)
    def _(i):
        rows = pl.ds(pl.multiple_of(i * 2 * count, 2 * count), 2 * count)
        mean = jnp.concatenate([mean_parts[2 * i], mean_parts[2 * i + 1]], axis=0)
        change = outer_momentum * momentum[rows, :] + mean
        new_momentum[rows, :] = change
        new_fragment[rows, :] = fragment[rows, :] - outer_rate * (mean + outer_momentum * change)


def rope_tables(positions, width):
    middle = width // 2
    frequency = rope_base ** (-2.0 * jnp.arange(middle, dtype=f32) / width)
    frequency = jnp.concatenate([frequency, frequency])
    angles = positions.astype(f32)[:, None] * frequency[None, :]
    return jnp.concatenate([jnp.cos(angles), jnp.sin(angles)], axis=0)


def swapped(bit):
    return [(index(x, y), index(x, y ^ bit)) for x in range(2) for y in range(4)]


def body(
    tokens,
    norm_gain,
    w_query,
    key_weight,
    value_weight,
    attention_gradient,
    global_fragment,
    momentum,
    local_fragment,
):
    rows = tokens[0]
    wq, wk, wv = w_query[0], key_weight[0], value_weight[0]
    me = lax.axis_index("tp")
    step_x = jnp.array([b[0] for b in BLOCKS], jnp.int32)
    step_y = jnp.array([b[1] for b in BLOCKS], jnp.int32)
    at = ((me // 4 + step_x) % 2) * 4 + (me % 4 + step_y + 4) % 4

    a00, b00 = call(
        norm_kernel, "norm", [shape(ROWS, A), shape(ROWS, B)], [rows, norm_gain], 10**6
    )
    a10 = across(a00)
    bm = up(b00)
    bp = down(b00)
    am = up(a00)
    ap = down(a00)
    b10 = across(b00)
    half = ROWS // 2
    b2l = up(bm[:half])
    b2h = down(bp[half:])
    (b2,) = call(join_kernel, "join", [shape(ROWS, B)], [b2l, b2h], 10**4)
    (pair,) = call(join_kernel, "pair", [shape(2 * ROWS, B)], [bm, bp], 10**4)
    b1 = across(pair)
    a1m = up(a10)
    a1p = down(a10)
    b12 = across(b2)
    a02 = up(am)
    a12 = down(a1p)

    parts_a = [a00, a10, am, ap, a1m, a1p, a02, a12]
    parts_b = [b00, b10, bm, bp, b1, b2, b12]
    weights = [wq, wk, wv]
    (first,) = call(
        functools.partial(project_kernel, 4),
        "project_first",
        [shape(512, 512, dtype=f32)],
        parts_a[:4] + parts_b[:4] + weights,
        2 * 512 * 512 * MODEL,
    )
    (second,) = call(
        functools.partial(project_kernel, 2),
        "project_second",
        [shape(256, 512, dtype=f32)],
        parts_a[4:6] + [b1] + weights,
        2 * 256 * 512 * MODEL,
    )
    (third,) = call(
        functools.partial(project_kernel, 2),
        "project_third",
        [shape(256, 512, dtype=f32)],
        parts_a[6:] + [b2, b12] + weights,
        2 * 256 * 512 * MODEL,
    )
    coarse = rope_tables(jnp.arange(0, SEQ, STRIDE), HEAD_SIZE)
    fine = rope_tables(jnp.arange(STRIDE), HEAD_SIZE)
    (grads,) = call(
        attention_kernel,
        "attention",
        [shape(SEQ, 512)],
        [at, first, second, third, coarse, fine, attention_gradient[0]],
        10 * SEQ * SEQ * 256,
        scratch=[
            pltpu.VMEM((SEQ, 256), bf16),
            pltpu.VMEM((SEQ, 128), bf16),
            pltpu.VMEM((SEQ, 128), bf16),
        ]
        + [pltpu.VMEM((SEQ, 128), f32)] * 4,
        smem=1,
    )
    far_low, far_high = call(
        far_back_kernel,
        "back_far",
        [shape(256, SH), shape(256, SA - SH)],
        [at, grads] + weights,
        2 * 512 * 256 * SA,
        smem=1,
    )
    x2, x1m, x0 = call(
        other_back_kernel,
        "back_other",
        [shape(ROWS, SB), shape(2 * ROWS, SB), shape(ROWS, SB)],
        [at, grads] + weights,
        2 * 512 * 512 * SB,
        smem=1,
    )
    near_low = up(far_low)
    near_high = down(far_high)
    r2 = across(x2)
    r1m = across(x1m)
    r0 = across(x0)
    up_low, up_high, down_low, down_high, own_a, q2, q1, qm, q0 = call(
        near_back_kernel,
        "back_near",
        [shape(256, SH), shape(256, SA - SH)] * 2 + [shape(256, SA)] + [shape(ROWS, SB)] * 4,
        [at, grads] + weights,
        2 * 512 * (768 * SA + 512 * SB),
        smem=1,
    )
    below_high = up(up_high)
    above_low = down(down_low)
    to_up, to_down = call(
        near_sum_kernel,
        "near_sum",
        [shape(3 * ROWS, SH)] * 2,
        [up_low, near_low, down_high, near_high, q2, r2],
        10**5,
    )
    below_low = up(to_up)
    above_high = down(to_down)
    b_up, b_down = call(
        b_sum_kernel,
        "b_sum",
        [shape(ROWS, SB)] * 2,
        [q1, qm, r1m, below_low, above_high],
        10**5,
    )
    from_below = up(b_up)
    from_above = down(b_down)
    own_sum, other_sum_a = call(
        a_sum_kernel,
        "a_sum",
        [shape(ROWS, SA, dtype=f32), shape(ROWS, SA)],
        [own_a, below_low, above_low, below_high, above_high],
        10**5,
    )
    from_x = across(other_sum_a)

    grad_wq, grad_wk, grad_wv, gain_part = call(
        weight_kernel,
        "weights",
        [shape(MODEL, 256), shape(MODEL, 128), shape(MODEL, 128), shape(1, MODEL, dtype=f32)],
        [at] + parts_a + parts_b + [grads] + weights + [norm_gain],
        2 * SEQ * 512 * MODEL,
        scratch=[pltpu.VMEM((SEQ, 512), bf16)],
        smem=1,
    )
    gain_row = [shape(1, MODEL, dtype=f32)]
    arrived_gain = lax.ppermute(gain_part, "tp", X_PAIRS)
    (gain_part,) = call(gain_sum_kernel, "e_sum0", gain_row, [gain_part, arrived_gain], 10**4)
    arrived_gain = lax.ppermute(gain_part, "tp", swapped(1))
    (gain_part,) = call(gain_sum_kernel, "e_sum1", gain_row, [gain_part, arrived_gain], 10**4)
    arrived_gain = lax.ppermute(gain_part, "tp", swapped(2))
    (grad_rows,) = call(
        token_kernel,
        "tokens",
        [shape(ROWS, MODEL)],
        [rows, norm_gain, own_sum, from_x, q0, r0, from_below, from_above],
        10**6,
    )

    replicas = lax.axis_size("rep")
    near = replicas // 2
    groups = [list(range(near)), list(range(near, replicas))]
    count = global_fragment.shape[0] // near
    (parts,) = call(
        share_kernel, "share", [shape(near, count, MODEL)], [local_fragment[0]], 10**4
    )
    arrived = lax.all_to_all(
        parts, "rep", split_axis=0, concat_axis=0, tiled=True, axis_index_groups=groups
    )
    offset = lax.axis_index("rep") % near * count
    global_rows = lax.dynamic_slice_in_dim(global_fragment, offset, count, 0)
    half_sum = jnp.sum(global_rows[None] - arrived.astype(f32), axis=0)
    other_sum = lax.ppermute(half_sum, "rep", [(i, (i + near) % replicas) for i in range(replicas)])
    (copies,) = call(
        spread_kernel, "spread", [shape(near, count, MODEL, dtype=f32)], [half_sum, other_sum], 10**4
    )
    mean = lax.all_to_all(
        copies, "rep", split_axis=0, concat_axis=0, tiled=True, axis_index_groups=groups
    )
    new_global, new_momentum, grad_gain = call(
        outer_kernel,
        "outer",
        [shape(*momentum.shape, dtype=f32)] * 2 + gain_row,
        [mean, global_fragment, momentum, gain_part, arrived_gain],
        10**5,
    )
    return (
        grad_wq[None],
        grad_wk[None],
        grad_wv[None],
        grad_gain,
        grad_rows[None],
        new_global,
        new_momentum,
    )


def solution(mesh):
    placed = (
        P("rep", "tp", None),
        P("rep", None),
        P("rep", None, "tp"),
        P("rep", None, "tp"),
        P("rep", None, "tp"),
        P("rep", None, "tp"),
        P("tp", None),
        P("tp", None),
        P("rep", "tp", None),
    )

    return jax.shard_map(
        body,
        mesh=mesh,
        in_specs=placed,
        out_specs=(
            P("rep", None, "tp"),
            P("rep", None, "tp"),
            P("rep", None, "tp"),
            P("rep", None),
            P("rep", "tp", None),
            P("tp", None),
            P("tp", None),
        ),
        check_vma=False,
    )
```

```python
import functools

import jax
import jax.numpy as jnp
from jax import lax
from jax.experimental import pallas as pl
from jax.experimental.pallas import tpu as pltpu
from jax.sharding import PartitionSpec as P


HEAD_SIZE = 128
A = 1792
MODEL = 3072
B = MODEL - A
SA = 1536
SB = MODEL - SA
SH = 768
SHB = 768
ROWS = 128
SEQ = 1024
TILE = 256
STRIDE = 32
STEP_A = 896
STEP_B = 640

epsilon = 1e-05
rope_base = 500000.0
outer_rate = 0.7
outer_momentum = 0.9


f32 = jnp.float32
bf16 = jnp.bfloat16
NT = (((1,), (1,)), ((), ()))
TN = (((0,), (0,)), ((), ()))
NN = (((1,), (0,)), ((), ()))

BLOCKS = ((0, 0), (1, 0), (0, -1), (0, 1), (1, -1), (1, 1), (0, 2), (1, 2))
WHERE = {block: at for at, block in enumerate(BLOCKS)}


def index(x, y):
    return x * 4 + y % 4


X_PAIRS = [(index(x, y), index(1 - x, y)) for x in range(2) for y in range(4)]
UP_PAIRS = [(index(x, y), index(x, y + 1)) for x in range(2) for y in range(4)]
DOWN_PAIRS = [(index(x, y), index(x, y - 1)) for x in range(2) for y in range(4)]


def across(value):
    return lax.ppermute(value, "tp", X_PAIRS)


def up(value):
    return lax.ppermute(value, "tp", UP_PAIRS)


def down(value):
    return lax.ppermute(value, "tp", DOWN_PAIRS)


def dot(a, b, dims):
    return lax.dot_general(a, b, dims, preferred_element_type=f32)


VMEM_LIMIT = {"attention": 16, "weights": 16, "project_first": 16}
VM = pl.BlockSpec(memory_space=pltpu.VMEM)
SM = pl.BlockSpec(memory_space=pltpu.SMEM)


def call(kernel, name, outs, ins, flops, scratch=(), smem=0):
    nbytes = sum(v.size * v.dtype.itemsize for v in ins) + sum(
        o.size * o.dtype.itemsize for o in outs
    )
    return pl.pallas_call(
        kernel,
        out_shape=tuple(outs),
        in_specs=[SM] * smem + [VM] * (len(ins) - smem),
        out_specs=tuple([VM] * len(outs)),
        scratch_shapes=list(scratch),
        cost_estimate=pl.CostEstimate(flops=flops, bytes_accessed=nbytes, transcendentals=0),
        compiler_params=pltpu.CompilerParams(vmem_limit_bytes=VMEM_LIMIT.get(name, 8) * 1024 * 1024),
    )(*ins)


def shape(*dims, dtype=bf16):
    return jax.ShapeDtypeStruct(dims, dtype)


def each_block(count, body):
    size = 32

    @pl.loop(0, count // size)
    def _(i):
        body(pl.ds(pl.multiple_of(i * size, size), size))


def norm_kernel(tokens, gain, part_a, part_b):
    def body(at):
        wide = tokens[at, :].astype(f32)
        inverse = lax.rsqrt(jnp.mean(wide * wide, axis=-1, keepdims=True) + epsilon)
        part_a[at, :] = (wide[:, :A] * inverse * gain[:, :A]).astype(bf16)
        part_b[at, :] = (wide[:, A:] * inverse * gain[:, A:]).astype(bf16)

    each_block(ROWS, body)


def project_kernel(n, *refs):
    wq, wk, wv, out = refs[-4:]
    rows_a = jnp.concatenate([r[...] for r in refs[:n]], axis=0)
    rows_b = jnp.concatenate([r[...] for r in refs[n:-4]], axis=0)
    out[:, :256] = dot(rows_a, wq[:A, :], NN) + dot(rows_b, wq[A:, :], NN)
    both = jnp.concatenate([wk[...], wv[...]], axis=1)
    out[:, 256:] = dot(rows_a, both[:A, :], NN) + dot(rows_b, both[A:, :], NN)


def join_kernel(low, high, out):
    out[: low.shape[0], :] = low[...]
    out[low.shape[0] :, :] = high[...]


def share_kernel(local, out):
    count = out.shape[1]
    for j in range(out.shape[0]):
        out[j] = local[j * count : (j + 1) * count, :]


def spread_kernel(mine, other, out):
    mean = (mine[...] + other[...]) / (2 * out.shape[0])
    for j in range(out.shape[0]):
        out[j] = mean


def sign_row():
    lane = lax.broadcasted_iota(jnp.int32, (1, HEAD_SIZE), 1)
    return jnp.where(lane < HEAD_SIZE // 2, -1.0, 1.0).astype(f32)


def attention_kernel(
    at, first, second, third, coarse, fine, grad_out, out, qs, ks, vs, dk, dv, cosine, sine
):
    sign = sign_row()
    scale = HEAD_SIZE ** (-0.5)
    fine_cos, fine_sin = fine[:STRIDE, :], fine[STRIDE:, :]
    for a in range(SEQ // STRIDE):
        c, s = coarse[a : a + 1, :], coarse[SEQ // STRIDE + a : SEQ // STRIDE + a + 1, :]
        cosine[a * STRIDE : (a + 1) * STRIDE, :] = c * fine_cos - s * fine_sin
        sine[a * STRIDE : (a + 1) * STRIDE, :] = s * fine_cos + c * fine_sin

    def rotate(v, c, s):
        return v * c + pltpu.roll(v, HEAD_SIZE // 2, 1) * (sign * s)

    def rotate_back(g, c, s):
        return g * c - pltpu.roll(g * s, HEAD_SIZE // 2, 1) * sign

    def place(source, base, j):
        here = pl.ds(pl.multiple_of(at[j] * ROWS, ROWS), ROWS)
        c, s = cosine[here, :], sine[here, :]
        block = source[pl.ds(pl.multiple_of(base, ROWS), ROWS), :]
        qs[here, :128] = rotate(block[:, :128], c, s).astype(bf16)
        qs[here, 128:] = rotate(block[:, 128:256], c, s).astype(bf16)
        ks[here, :] = rotate(block[:, 256:384], c, s).astype(bf16)
        vs[here, :] = block[:, 384:].astype(bf16)

    @pl.loop(0, 4)
    def _(j):
        place(first, j * ROWS, j)

    @pl.loop(0, 2)
    def _(j):
        place(second, j * ROWS, j + 4)
        place(third, j * ROWS, j + 6)

    dk[...] = jnp.zeros_like(dk)
    dv[...] = jnp.zeros_like(dv)
    key_at = lax.broadcasted_iota(jnp.int32, (TILE, TILE), 0)
    query_at = lax.broadcasted_iota(jnp.int32, (TILE, TILE), 1)
    allowed = key_at <= query_at
    for i in range(SEQ // TILE):
        lo, hi = i * TILE, (i + 1) * TILE

        keys, values = ks[:hi, :], vs[:hi, :]
        for h in range(2):
            cols = slice(h * 128, (h + 1) * 128)
            q, g = qs[lo:hi, cols], grad_out[lo:hi, cols]
            scores = dot(keys, q, NT) * scale
            last = jnp.where(allowed, scores[lo:, :], -jnp.inf)
            scores = jnp.concatenate([scores[:lo, :], last], axis=0) if i else last
            powers = jnp.exp(scores - jnp.max(scores, axis=0, keepdims=True))
            probability = powers * (1.0 / jnp.sum(powers, axis=0, keepdims=True))
            dv[:hi, :] += dot(probability.astype(bf16), g, NN)
            grad_prob = dot(values, g, NT)
            row = jnp.sum(grad_prob * probability, axis=0, keepdims=True)
            grad_score = (probability * (grad_prob - row) * scale).astype(bf16)
            dk[:hi, :] += dot(grad_score, q, NN)
            dq = dot(grad_score, keys, TN)
            out[lo:hi, cols] = rotate_back(dq, cosine[lo:hi, :], sine[lo:hi, :]).astype(bf16)

    out[:, 256:384] = rotate_back(dk[...], cosine[...], sine[...]).astype(bf16)
    out[:, 384:] = dv[...].astype(bf16)


def rows_of(at, ref, block):
    return ref[pl.ds(pl.multiple_of(at[WHERE[block]] * ROWS, ROWS), ROWS), :]


def back_tile(rows, wq, wk, wv, cols):
    both = jnp.concatenate([wk[cols, :], wv[cols, :]], axis=1)
    return (dot(rows[:, :256], wq[cols, :], NT) + dot(rows[:, 256:], both, NT)).astype(bf16)


def columns(i, base=0):
    return pl.ds(pl.multiple_of(i * TILE + base, TILE), TILE)


def far_back_kernel(at, grads, wq, wk, wv, far_low, far_high):
    far = jnp.concatenate([rows_of(at, grads, (0, 2)), rows_of(at, grads, (1, 2))], axis=0)

    @pl.loop(0, SH // TILE)
    def _(i):
        far_low[:, columns(i)] = back_tile(far, wq, wk, wv, columns(i))
        far_high[:, columns(i)] = back_tile(far, wq, wk, wv, columns(i, SH))


def other_back_kernel(at, grads, wq, wk, wv, x2, x1m, x0):
    other = jnp.concatenate([rows_of(at, grads, (1, d)) for d in (2, 1, -1, 0)], axis=0)

    @pl.loop(0, SHB // TILE)
    def _(i):
        for base in (0, SHB):
            tile = back_tile(other, wq, wk, wv, columns(i, SA + base))
            x2[:, columns(i, base)] = tile[:ROWS, :]
            x1m[:, columns(i, base)] = tile[ROWS : 3 * ROWS, :]
            x0[:, columns(i, base)] = tile[3 * ROWS :, :]


def near_back_kernel(
    at, grads, wq, wk, wv, up_low, up_high, down_low, down_high, own_a, q2, q1, qm, q0
):
    near = jnp.concatenate(
        [rows_of(at, grads, (x, d)) for d in (1, -1, 0) for x in (0, 1)], axis=0
    )
    mine = jnp.concatenate([rows_of(at, grads, (0, d)) for d in (2, 1, -1, 0)], axis=0)

    @pl.loop(0, SH // TILE)
    def _(i):
        for base, above, below in ((0, up_low, down_low), (SH, up_high, down_high)):
            tile = back_tile(near, wq, wk, wv, columns(i, base))
            above[:, columns(i)] = tile[:256, :]
            below[:, columns(i)] = tile[256:512, :]
            own_a[:, columns(i, base)] = tile[512:, :]

    @pl.loop(0, SHB // TILE)
    def _(i):
        for base in (0, SHB):
            tile = back_tile(mine, wq, wk, wv, columns(i, SA + base))
            for n, ref in enumerate((q2, q1, qm, q0)):
                ref[:, columns(i, base)] = tile[n * ROWS : (n + 1) * ROWS, :]


def weight_kernel(at, *refs):
    parts_a, parts_b = refs[:8], refs[8:15]
    grads, wq, wk, wv, dwq, dwk, dwv, gain_part, ordered = refs[15:]
    for j in range(8):
        ordered[j * ROWS : (j + 1) * ROWS, :] = grads[
            pl.ds(pl.multiple_of(at[j] * ROWS, ROWS), ROWS), :
        ]

    def tile(rows, to, size):
        product = dot(rows, ordered[...], TN)
        where = pl.ds(to, size)
        dwq[where, :] = product[:, :256].astype(bf16)
        dwk[where, :] = product[:, 256:384].astype(bf16)
        dwv[where, :] = product[:, 384:].astype(bf16)
        total = (
            product[:, :128] * wq[where, :128].astype(f32)
            + product[:, 128:256] * wq[where, 128:].astype(f32)
            + product[:, 256:384] * wk[where, :].astype(f32)
            + product[:, 384:] * wv[where, :].astype(f32)
        )
        gain_part[:, where] = jnp.sum(total.T, axis=0, keepdims=True)

    @pl.loop(0, A // STEP_A)
    def _(i):
        col = pl.multiple_of(i * STEP_A, 128)
        rows = [r[:, pl.ds(col, STEP_A)] for r in parts_a]
        tile(jnp.concatenate(rows, axis=0), col, STEP_A)

    @pl.loop(0, B // STEP_B)
    def _(i):
        col = pl.multiple_of(i * STEP_B, 128)
        rows = [r[:, pl.ds(col, STEP_B)] for r in parts_b]
        tile(jnp.concatenate(rows, axis=0), pl.multiple_of(A + col, 128), STEP_B)


def near_sum_kernel(up_low, near_low, down_high, near_high, mine, arrived, to_up, to_down):
    count = 2 * ROWS
    to_up[:count, :] = (up_low[...].astype(f32) + near_low[...].astype(f32)).astype(bf16)
    to_down[:count, :] = (down_high[...].astype(f32) + near_high[...].astype(f32)).astype(bf16)
    total = (mine[...].astype(f32) + arrived[...].astype(f32)).astype(bf16)
    to_up[count:, :] = total[:, :SHB]
    to_down[count:, :] = total[:, SHB:]


def b_sum_kernel(q1, qm, r, near_low, near_high, to_up, to_down):
    low, high = slice(0, SHB), slice(SHB, SB)
    size = 32

    @pl.loop(0, ROWS // size)
    def _(i):
        at = pl.ds(pl.multiple_of(i * size, size), size)
        below = pl.ds(pl.multiple_of(i * size + ROWS, size), size)
        near = pl.ds(pl.multiple_of(i * size + 2 * ROWS, size), size)

        def total(q, rows, cols):
            return q[at, cols].astype(f32) + r[rows, cols].astype(f32)

        to_up[at, low] = (total(q1, at, low) + near_low[near, :].astype(f32)).astype(bf16)
        to_up[at, high] = total(q1, at, high).astype(bf16)
        to_down[at, low] = total(qm, below, low).astype(bf16)
        to_down[at, high] = (total(qm, below, high) + near_high[near, :].astype(f32)).astype(bf16)


def a_sum_kernel(own, below_low, above_low, below_high, above_high, mine, other):
    size = 32

    @pl.loop(0, ROWS // size)
    def _(i):
        at = pl.ds(pl.multiple_of(i * size, size), size)
        far = pl.ds(pl.multiple_of(i * size + ROWS, size), size)
        for cols, below, above in (
            (slice(0, SH), below_low, above_low),
            (slice(SH, SA), below_high, above_high),
        ):

            def total(rows):
                return (
                    own[rows, cols].astype(f32)
                    + below[rows, :].astype(f32)
                    + above[rows, :].astype(f32)
                )

            mine[at, cols] = total(at)
            other[at, cols] = total(far).astype(bf16)


def gain_sum_kernel(mine, arrived, out):
    out[...] = mine[...] + arrived[...]


def token_kernel(
    tokens, gain, own_a, from_x, q0, r0, from_below, from_above, part, other_part, out, grad_gain
):
    grad_gain[...] = (part[...] + other_part[...]) / gain[...]

    def body(at):
        wide = tokens[at, :].astype(f32)
        inverse = lax.rsqrt(jnp.mean(wide * wide, axis=-1, keepdims=True) + epsilon)
        hat = wide * inverse
        sum_a = own_a[at, :] + from_x[at, :].astype(f32)
        sum_b = (q0[at, :].astype(f32) + r0[at, :].astype(f32)) + (
            from_below[at, :].astype(f32) + from_above[at, :].astype(f32)
        )
        scaled_a = sum_a * gain[:, :SA]
        scaled_b = sum_b * gain[:, SA:]
        mean = (
            jnp.sum(scaled_a * hat[:, :SA], axis=-1, keepdims=True)
            + jnp.sum(scaled_b * hat[:, SA:], axis=-1, keepdims=True)
        ) / MODEL
        out[at, :SA] = (inverse * (scaled_a - hat[:, :SA] * mean)).astype(bf16)
        out[at, SA:] = (inverse * (scaled_b - hat[:, SA:] * mean)).astype(bf16)

    each_block(ROWS, body)


def outer_kernel(mean_parts, fragment, momentum, new_fragment, new_momentum):
    count = mean_parts.shape[1]

    @pl.loop(0, mean_parts.shape[0] // 2)
    def _(i):
        rows = pl.ds(pl.multiple_of(i * 2 * count, 2 * count), 2 * count)
        mean = jnp.concatenate([mean_parts[2 * i], mean_parts[2 * i + 1]], axis=0)
        change = outer_momentum * momentum[rows, :] + mean
        new_momentum[rows, :] = change
        new_fragment[rows, :] = fragment[rows, :] - outer_rate * (mean + outer_momentum * change)


def rope_tables(positions, width):
    middle = width // 2
    frequency = rope_base ** (-2.0 * jnp.arange(middle, dtype=f32) / width)
    frequency = jnp.concatenate([frequency, frequency])
    angles = positions.astype(f32)[:, None] * frequency[None, :]
    return jnp.concatenate([jnp.cos(angles), jnp.sin(angles)], axis=0)


def swapped(bit):
    return [(index(x, y), index(x, y ^ bit)) for x in range(2) for y in range(4)]


def body(
    tokens,
    norm_gain,
    w_query,
    key_weight,
    value_weight,
    attention_gradient,
    global_fragment,
    momentum,
    local_fragment,
):
    rows = tokens[0]
    wq, wk, wv = w_query[0], key_weight[0], value_weight[0]
    me = lax.axis_index("tp")
    step_x = jnp.array([b[0] for b in BLOCKS], jnp.int32)
    step_y = jnp.array([b[1] for b in BLOCKS], jnp.int32)
    at = ((me // 4 + step_x) % 2) * 4 + (me % 4 + step_y + 4) % 4

    a00, b00 = call(
        norm_kernel, "norm", [shape(ROWS, A), shape(ROWS, B)], [rows, norm_gain], 10**6
    )
    a10 = across(a00)
    bm = up(b00)
    bp = down(b00)
    am = up(a00)
    ap = down(a00)
    b10 = across(b00)
    half = ROWS // 2
    b2l = up(bm[:half])
    b2h = down(bp[half:])
    (b2,) = call(join_kernel, "join", [shape(ROWS, B)], [b2l, b2h], 10**4)
    (pair,) = call(join_kernel, "pair", [shape(2 * ROWS, B)], [bm, bp], 10**4)
    b1 = across(pair)
    a1m = up(a10)
    a1p = down(a10)
    b12 = across(b2)
    a02 = up(am)
    a12 = down(a1p)

    parts_a = [a00, a10, am, ap, a1m, a1p, a02, a12]
    parts_b = [b00, b10, bm, bp, b1, b2, b12]
    weights = [wq, wk, wv]
    (first,) = call(
        functools.partial(project_kernel, 4),
        "project_first",
        [shape(512, 512, dtype=f32)],
        parts_a[:4] + parts_b[:4] + weights,
        2 * 512 * 512 * MODEL,
    )
    (second,) = call(
        functools.partial(project_kernel, 2),
        "project_second",
        [shape(256, 512, dtype=f32)],
        parts_a[4:6] + [b1] + weights,
        2 * 256 * 512 * MODEL,
    )
    (third,) = call(
        functools.partial(project_kernel, 2),
        "project_third",
        [shape(256, 512, dtype=f32)],
        parts_a[6:] + [b2, b12] + weights,
        2 * 256 * 512 * MODEL,
    )
    coarse = rope_tables(jnp.arange(0, SEQ, STRIDE), HEAD_SIZE)
    fine = rope_tables(jnp.arange(STRIDE), HEAD_SIZE)
    (grads,) = call(
        attention_kernel,
        "attention",
        [shape(SEQ, 512)],
        [at, first, second, third, coarse, fine, attention_gradient[0]],
        10 * SEQ * SEQ * 256,
        scratch=[
            pltpu.VMEM((SEQ, 256), bf16),
            pltpu.VMEM((SEQ, 128), bf16),
            pltpu.VMEM((SEQ, 128), bf16),
        ]
        + [pltpu.VMEM((SEQ, 128), f32)] * 4,
        smem=1,
    )
    far_low, far_high = call(
        far_back_kernel,
        "back_far",
        [shape(256, SH), shape(256, SA - SH)],
        [at, grads] + weights,
        2 * 512 * 256 * SA,
        smem=1,
    )
    x2, x1m, x0 = call(
        other_back_kernel,
        "back_other",
        [shape(ROWS, SB), shape(2 * ROWS, SB), shape(ROWS, SB)],
        [at, grads] + weights,
        2 * 512 * 512 * SB,
        smem=1,
    )
    near_low = up(far_low)
    near_high = down(far_high)
    r2 = across(x2)
    r1m = across(x1m)
    r0 = across(x0)
    up_low, up_high, down_low, down_high, own_a, q2, q1, qm, q0 = call(
        near_back_kernel,
        "back_near",
        [shape(256, SH), shape(256, SA - SH)] * 2 + [shape(256, SA)] + [shape(ROWS, SB)] * 4,
        [at, grads] + weights,
        2 * 512 * (768 * SA + 512 * SB),
        smem=1,
    )
    below_high = up(up_high)
    above_low = down(down_low)
    to_up, to_down = call(
        near_sum_kernel,
        "near_sum",
        [shape(3 * ROWS, SH)] * 2,
        [up_low, near_low, down_high, near_high, q2, r2],
        10**5,
    )
    below_low = up(to_up)
    above_high = down(to_down)
    b_up, b_down = call(
        b_sum_kernel,
        "b_sum",
        [shape(ROWS, SB)] * 2,
        [q1, qm, r1m, below_low, above_high],
        10**5,
    )
    from_below = up(b_up)
    from_above = down(b_down)
    own_sum, other_sum_a = call(
        a_sum_kernel,
        "a_sum",
        [shape(ROWS, SA, dtype=f32), shape(ROWS, SA)],
        [own_a, below_low, above_low, below_high, above_high],
        10**5,
    )
    from_x = across(other_sum_a)

    grad_wq, grad_wk, grad_wv, gain_part = call(
        weight_kernel,
        "weights",
        [shape(MODEL, 256), shape(MODEL, 128), shape(MODEL, 128), shape(1, MODEL, dtype=f32)],
        [at] + parts_a + parts_b + [grads] + weights,
        2 * SEQ * 512 * MODEL,
        scratch=[pltpu.VMEM((SEQ, 512), bf16)],
        smem=1,
    )
    gain_row = [shape(1, MODEL, dtype=f32)]
    arrived_gain = lax.ppermute(gain_part, "tp", X_PAIRS)
    (gain_part,) = call(gain_sum_kernel, "e_sum0", gain_row, [gain_part, arrived_gain], 10**4)
    arrived_gain = lax.ppermute(gain_part, "tp", swapped(1))
    (gain_part,) = call(gain_sum_kernel, "e_sum1", gain_row, [gain_part, arrived_gain], 10**4)
    arrived_gain = lax.ppermute(gain_part, "tp", swapped(2))
    grad_rows, grad_gain = call(
        token_kernel,
        "tokens",
        [shape(ROWS, MODEL)] + gain_row,
        [rows, norm_gain, own_sum, from_x, q0, r0, from_below, from_above]
        + [gain_part, arrived_gain],
        10**6,
    )

    replicas = lax.axis_size("rep")
    near = replicas // 2
    groups = [list(range(near)), list(range(near, replicas))]
    count = global_fragment.shape[0] // near
    (parts,) = call(
        share_kernel, "share", [shape(near, count, MODEL)], [local_fragment[0]], 10**4
    )
    arrived = lax.all_to_all(
        parts, "rep", split_axis=0, concat_axis=0, tiled=True, axis_index_groups=groups
    )
    offset = lax.axis_index("rep") % near * count
    global_rows = lax.dynamic_slice_in_dim(global_fragment, offset, count, 0)
    half_sum = jnp.sum(global_rows[None] - arrived.astype(f32), axis=0)
    other_sum = lax.ppermute(half_sum, "rep", [(i, (i + near) % replicas) for i in range(replicas)])
    (copies,) = call(
        spread_kernel, "spread", [shape(near, count, MODEL, dtype=f32)], [half_sum, other_sum], 10**4
    )
    mean = lax.all_to_all(
        copies, "rep", split_axis=0, concat_axis=0, tiled=True, axis_index_groups=groups
    )
    new_global, new_momentum = call(
        outer_kernel,
        "outer",
        [shape(*momentum.shape, dtype=f32)] * 2,
        [mean, global_fragment, momentum],
        10**5,
    )
    return (
        grad_wq[None],
        grad_wk[None],
        grad_wv[None],
        grad_gain,
        grad_rows[None],
        new_global,
        new_momentum,
    )


def solution(mesh):
    placed = (
        P("rep", "tp", None),
        P("rep", None),
        P("rep", None, "tp"),
        P("rep", None, "tp"),
        P("rep", None, "tp"),
        P("rep", None, "tp"),
        P("tp", None),
        P("tp", None),
        P("rep", "tp", None),
    )

    return jax.shard_map(
        body,
        mesh=mesh,
        in_specs=placed,
        out_specs=(
            P("rep", None, "tp"),
            P("rep", None, "tp"),
            P("rep", None, "tp"),
            P("rep", None),
            P("rep", "tp", None),
            P("tp", None),
            P("tp", None),
        ),
        check_vma=False,
    )
```
